256 devices in a mesh: ctx: 64 (over y, z, core), head: 4 (over x).
Axes of the slice: x: 4, y: 4, z: 8, core: 2. Of those that a mesh axis runs over, the one named last changes fastest.
Arguments:
- queries: bfloat16 [8192, 2048], P('ctx', 'head'), may hold values from -6 to 6
- keys: bfloat16 [8192, 2048], P('ctx', 'head'), may hold values from -6 to 6
- values: bfloat16 [8192, 4096], P('ctx', 'head'), may hold values from -6 to 6
- out_gate: bfloat16 [8192, 4096], P('ctx', 'head'), may hold values from -6 to 6
- log_decay: float32 [8192, 32], P('ctx', 'head'), may hold values from -1.5 to 0, as said below
- write_strength: float32 [8192, 32], P('ctx', 'head'), may hold values from 0 to 1
- segment_ids: int32 [8192], P('ctx'), may hold values from 0 to 3, never falling along the last dimension, each value on 1 to 4096 neighbouring positions
- head_order: int32 [32], replicated, may hold values from 0 to 31, each once
- out_weight: bfloat16 [4096, 2048], P('head'), may hold values from -0.09375 to 0.09375
Outputs:
- layer_out: bfloat16 [8192, 2048], P(('ctx', 'head'))
- decode_states: float32 [32, 16384], P('head', 'ctx')
The draws below stay inside these ranges and needn't reach their ends.
Inputs may be any that keep to these rules, and one draw needn't show every extreme that they name: `log_decay`: Negative.
All inputs are finite; a program needn't handle non-finite values.
Results may differ from the reference program's by a relative error of at most 0.0049.
Values may be sent and summed in bfloat16 or wider, within the bound.
No kernel may reach another device: no remote copies, remote signals or barrier semaphores. Data moves between devices by JAX's collectives and lax.ppermute only.
A program may use at most 192 MiB of HBM per device.

```python
import math
import jax
import jax.numpy as jnp
import numpy as np
from jax import lax

D = 2048
HK = 16
VALUE_HEADS = 32
DK = 128
DV = 128
BLOCK = 64
TOK_DEV = 128
WINDOW_TOKENS = 8192
N_CTX = 64


def head_kinds(key):
    kind_key = jax.random.fold_in(key, 7001)
    slow_share = 5
    return jax.random.randint(kind_key, (VALUE_HEADS,), 0, 10) < slow_share


def draw_log_decay(key, part):
    slow_heads = head_kinds(key)
    random_subkeys = jax.random.split(jax.random.fold_in(key, 7002), 6)
    slow_rate = jnp.exp(jax.random.uniform(random_subkeys[0], (VALUE_HEADS,), minval=math.log(0.2), maxval=0.0)) * math.log(10.0) / WINDOW_TOKENS
    fast_rate = 1.0 / jax.random.uniform(random_subkeys[1], (VALUE_HEADS,), minval=30.0, maxval=50.0)
    head_rate = jnp.where(slow_heads, slow_rate, fast_rate)
    block_factor = jnp.exp(jax.random.uniform(random_subkeys[2], (WINDOW_TOKENS // TOK_DEV, VALUE_HEADS), minval=math.log(0.5), maxval=math.log(2.0)))
    block_factor = jnp.repeat(block_factor, TOK_DEV, axis=0)
    token_factor = jnp.exp(jax.random.uniform(random_subkeys[3], (WINDOW_TOKENS, VALUE_HEADS), minval=math.log(0.5), maxval=math.log(2.0)))
    surge_position = jax.random.randint(random_subkeys[4], (3, VALUE_HEADS), 0, WINDOW_TOKENS)
    token_positions = jnp.arange(WINDOW_TOKENS)[:, None, None]
    surge_active = jnp.any(token_positions == surge_position[None, :, :], axis=1)
    surge_falloff = jnp.log(jax.random.uniform(random_subkeys[5], (WINDOW_TOKENS, VALUE_HEADS), minval=0.5, maxval=0.8))
    smoothed_rows = -head_rate[None, :] * block_factor * token_factor
    return (smoothed_rows + jnp.where(surge_active, surge_falloff, 0.0)).astype(jnp.float32)


def draw_write_strength(key, part):
    slow_heads = head_kinds(key)
    random_subkeys = jax.random.split(jax.random.fold_in(key, 7003), 2)
    slow_value = jnp.exp(jax.random.uniform(random_subkeys[0], (WINDOW_TOKENS, VALUE_HEADS), minval=math.log(0.1), maxval=0.0)) * 0.8 * DK / WINDOW_TOKENS
    fast_value = jax.random.uniform(random_subkeys[1], (WINDOW_TOKENS, VALUE_HEADS), minval=0.2, maxval=0.95)
    return jnp.where(slow_heads[None, :], slow_value, fast_value).astype(jnp.float32)


def block_scale(key, extent, cuts, low, top_value):
    gain = 1.0
    for axis_at, blocks in cuts:
        steps = jax.random.uniform(jax.random.fold_in(jax.random.fold_in(key, 6), axis_at), (blocks,), jnp.float32, low / len(cuts), top_value / len(cuts))
        gain = gain * jnp.repeat(jnp.exp(steps), extent[axis_at] // blocks).reshape((-1,) + (1,) * (len(extent) - 1 - axis_at))
    return gain


def profile(amount, total, limit, skew):
    loads = [(1 << 20) // math.isqrt(rank ** skew) + 1 for rank in range(2, amount + 1)]
    rest, holding = total - limit - (amount - 1), [1] * (amount - 1)
    while rest > 0:
        candidates = [i for i in range(amount - 1) if holding[i] < limit]
        mass, remaining = sum([loads[i] for i in candidates]), rest
        for i in candidates:
            more = min(limit - holding[i], max(1, remaining * loads[i] // mass), rest)
            holding[i] = holding[i] + more
            rest = rest - more
    return np.array([limit] + holding)


def uneven(rng, amount, total, reach, slope):
    if amount == 2:
        one = jax.random.randint(rng, (), max(1, total - reach), min(reach, total - 1) + 1)
        return jnp.stack([one, total - one])
    tallies = jnp.asarray(profile(amount, total, reach, slope), jnp.int32)
    couples = (amount - 1) // 2
    source_of, sink = tallies[1:1 + 2 * couples:2], tallies[2:2 + 2 * couples:2]
    margin = jnp.minimum(source_of - 1, reach - sink)
    passed = jax.random.randint(jax.random.fold_in(rng, 1), (couples,), 0, 1 << 20) % (margin + 1)
    tallies = tallies.at[1:1 + 2 * couples:2].set(source_of - passed).at[2:2 + 2 * couples:2].set(sink + passed)
    return tallies[jax.random.permutation(jax.random.fold_in(rng, 2), amount)]


def gaussian(stream_key, shape, deviation, reach, cuts=(), held_as=jnp.bfloat16):
    values = deviation * jax.random.normal(stream_key, shape, jnp.float32)
    if cuts:
        values = values * block_scale(stream_key, shape, cuts, -0.22, 0.18)
    return jnp.clip(values, -reach, reach).astype(held_as)


def setup_inputs(seed: int = 0) -> dict:
    key_of = jax.random.split(jax.random.key(seed), 10)
    queries = gaussian(key_of[0], (WINDOW_TOKENS, HK * DK), 1.0, 6.0, ((0, 64), (1, 4)))
    keys = gaussian(key_of[1], (WINDOW_TOKENS, HK * DK), 1.0, 6.0, ((0, 64), (1, 4)))
    values = gaussian(key_of[2], (WINDOW_TOKENS, VALUE_HEADS * DV), 1.0, 6.0, ((0, 64), (1, 4)))
    out_gate = gaussian(key_of[3], (WINDOW_TOKENS, VALUE_HEADS * DV), 1.0, 6.0, ((0, 64), (1, 4)))
    log_decay = draw_log_decay(jax.random.fold_in(key_of[9], 71), 0)
    write_strength = draw_write_strength(jax.random.fold_in(key_of[9], 71), 0)
    segment_ids = jnp.searchsorted(jnp.cumsum(uneven(key_of[6], max(3, N_CTX // 16), WINDOW_TOKENS, WINDOW_TOKENS // 2, 0)), jnp.arange(WINDOW_TOKENS), side="right").astype(jnp.int32)
    head_order = jax.random.permutation(key_of[7], VALUE_HEADS).astype(jnp.int32)
    out_weight = gaussian(key_of[8], (VALUE_HEADS * DV, D), (VALUE_HEADS * DV) ** -0.5, 0.09375, ((0, 4),))
    return dict(queries=queries, keys=keys, values=values, out_gate=out_gate, log_decay=log_decay, write_strength=write_strength, segment_ids=segment_ids, head_order=head_order, out_weight=out_weight)


highest = lax.Precision.HIGHEST
norm_eps = 1e-06

def product(form, left, right):
    return jnp.einsum(form, left, right, precision=highest)

def unit_rows(raw_rows, scaling):
    widened = raw_rows.astype(jnp.float32)
    return widened * lax.rsqrt(lax.optimization_barrier(jnp.sum(widened * widened, axis=-1, keepdims=True)) + norm_eps) * scaling

def gated_norm(attention, gate_rows):
    mean_square = lax.optimization_barrier(jnp.mean(attention * attention, axis=-1, keepdims=True))
    gated = attention * lax.rsqrt(mean_square + norm_eps) * jax.nn.silu(gate_rows.astype(jnp.float32))
    return gated.astype(jnp.bfloat16)

def inverse_unit_lower(coupling):
    block_size = coupling.shape[-1]
    identity_matrix = jnp.eye(block_size, dtype=jnp.float32)
    inverse = identity_matrix - coupling
    squared = coupling
    for doubling in range(block_size.bit_length() - 2):
        squared = product('...ij,...jk->...ik', squared, squared)
        inverse = product('...ij,...jk->...ik', inverse, identity_matrix + squared)
    return inverse

def block_parts(query_part, key_part, value_part, decay_rows, strength_rows, doc_rows, doc_before):
    block_size = doc_rows.shape[-1]
    token_positions = jnp.arange(block_size)
    causal = token_positions[:, None] >= token_positions[None, :]
    strict = token_positions[:, None] > token_positions[None, :]
    same_doc = (doc_rows[..., :, None] == doc_rows[..., None, :]) & causal
    continues = doc_rows == doc_before[..., None]
    cumulative = jnp.cumsum(decay_rows, axis=-1)
    decay_gap = cumulative[..., :, None] - cumulative[..., None, :]
    mixing = jnp.where(same_doc[..., None, :, :], jnp.exp(jnp.minimum(decay_gap, 0.0)), 0.0)
    entry_decay = jnp.where(continues[..., None, :], jnp.exp(cumulative), 0.0)
    key_intersection = product('...id,...jd->...ij', key_part, key_part)
    coupling = jnp.where(strict, strength_rows[..., :, None] * mixing * key_intersection, 0.0)
    inverse = inverse_unit_lower(coupling)
    weighted = product('...ij,...jd->...id', inverse, (strength_rows * entry_decay)[..., None] * key_part)
    pseudo_values = product('...ij,...jd->...id', inverse, strength_rows[..., None] * value_part)
    masked_scores = mixing * product('...id,...jd->...ij', query_part, key_part)
    local_out = product('...ij,...jd->...id', masked_scores, pseudo_values)
    state_read = entry_decay[..., None] * query_part - product('...ij,...jd->...id', masked_scores, weighted)
    last_keys = mixing[..., -1, :, None] * key_part
    identity_map = jnp.eye(key_part.shape[-1], dtype=jnp.float32)
    transition = entry_decay[..., -1, None, None] * identity_map - product('...jd,...je->...de', last_keys, weighted)
    written = product('...jd,...je->...de', last_keys, pseudo_values)
    return (local_out, state_read, transition, written)

def reference(queries, keys, values, out_gate, log_decay, write_strength, segment_ids, head_order, out_weight):
    tokens = queries.shape[0]
    blocks = tokens // BLOCK
    group_size = VALUE_HEADS // HK
    doc_blocks = segment_ids.reshape(blocks, BLOCK)
    doc_before = jnp.concatenate([doc_blocks[:1, 0], doc_blocks[:-1, -1]]).astype(jnp.int32)

    def advance(carried, pieces):
        query_raw, key_raw, value_raw, gate_raw, decay_raw, strength_raw, doc_rows, doc_prior = pieces
        query_part = jnp.repeat(unit_rows(query_raw.reshape(BLOCK, HK, DK), DK ** (-0.5)), group_size, axis=1).transpose(1, 0, 2)
        key_part = jnp.repeat(unit_rows(key_raw.reshape(BLOCK, HK, DK), 1.0), group_size, axis=1).transpose(1, 0, 2)
        value_part = value_raw.reshape(BLOCK, VALUE_HEADS, DV).astype(jnp.float32).transpose(1, 0, 2)
        local_out, state_read, transition, written = block_parts(query_part, key_part, value_part, decay_raw.T, strength_raw.T, doc_rows, doc_prior)
        attention = local_out + product('hid,hde->hie', state_read, carried)
        normed = gated_norm(attention.transpose(1, 0, 2), gate_raw.reshape(BLOCK, VALUE_HEADS, DV)).reshape(BLOCK, VALUE_HEADS * DV)
        projected = jnp.dot(normed, out_weight, preferred_element_type=jnp.float32).astype(jnp.bfloat16)
        return (product('hde,hef->hdf', transition, carried) + written, projected)
    inputs = (queries.reshape(blocks, BLOCK, HK * DK), keys.reshape(blocks, BLOCK, HK * DK), values.reshape(blocks, BLOCK, VALUE_HEADS * DV), out_gate.reshape(blocks, BLOCK, VALUE_HEADS * DV), log_decay.reshape(blocks, BLOCK, VALUE_HEADS), write_strength.reshape(blocks, BLOCK, VALUE_HEADS), doc_blocks, doc_before)
    final_state, outputs = lax.scan(advance, jnp.zeros((VALUE_HEADS, DK, DV), jnp.float32), inputs)
    decode_states = jnp.take(final_state.reshape(VALUE_HEADS, DK * DV), head_order, axis=0)
    return (outputs.reshape(tokens, D), decode_states)
```

```python
import jax
import jax.numpy as jnp
from jax import lax
from jax.experimental import pallas as pl
from jax.experimental.pallas import tpu as pltpu
from jax.sharding import PartitionSpec as P

f32 = jnp.float32
bf16 = jnp.bfloat16
DK = 128
DV = 128
N = 128
ROWS = N + 16
EPS = 1e-06


def mm(a, b):
    return jnp.dot(a, b, preferred_element_type=f32)


def split(x):
    hi = x.astype(bf16)
    return hi, (x - hi.astype(f32)).astype(bf16)


def mm_left(a, b):
    hi, lo = split(a)
    return mm(jnp.concatenate([hi, lo], 1), jnp.concatenate([b, b], 0))


def mm_right(a, b):
    hi, lo = split(b)
    return mm(jnp.concatenate([a, a], 1), jnp.concatenate([hi, lo], 0))


def mm_both(a, b):
    ah, al = split(a)
    bh, bl = split(b)
    return mm(jnp.concatenate([ah, al], 1), jnp.concatenate([bh, bh], 0)) + mm(ah, bl)


def iota(shape, axis):
    return lax.broadcasted_iota(jnp.int32, shape, axis)


def places():
    ctx = lax.axis_index("ctx")
    return ctx % 2, (ctx // 2) % 4, (ctx // 8) % 2, ctx // 16


def lines(shape, values):
    row = iota(shape, 0)
    out = jnp.zeros(shape, f32)
    for i, value in enumerate(values):
        out = jnp.where(row == i, jnp.broadcast_to(value[:, :1], shape), out)
    return out


def pack_wide(ref, at, c, d, b, first, last):
    ref[at + (pl.ds(0, N), pl.ds(0, DK))] = d
    ref[at + (pl.ds(0, N), pl.ds(DK, DV))] = b
    ref[at + (pl.ds(N, 8), slice(None))] = lines((8, 256), (c, first, last))


def parse_wide(block):
    tail = block[N:, :DK]
    return tail[0:1], block[:N, :DK], block[:N, DK:], tail[1:2], tail[2:3]


def pack(ref, c, d, b, first, last):
    c0 = c.astype(bf16).astype(f32)
    c1 = (c - c0).astype(bf16).astype(f32)
    ref[:N, :DK] = d.astype(bf16)
    hi = b.astype(bf16)
    ref[:N, DK : 2 * DK] = hi
    if ref.shape[1] > 2 * DK:
        ref[:N, 2 * DK :] = (b - hi.astype(f32)).astype(bf16)
    ref[N:] = lines((16, ref.shape[1]), (c0, c1, c - c0 - c1, first, last)).astype(bf16)


def parse(block):
    tail = block[N:, :DK].astype(f32)
    c = tail[0:1] + tail[1:2] + tail[2:3]
    b = block[:N, DK : 2 * DK].astype(f32)
    if block.shape[1] > 2 * DK:
        b = b + block[:N, 2 * DK :].astype(f32)
    return c, block[:N, :DK], b, tail[3:4], tail[4:5]


def times(d, x):
    return mm_right(d, x) if d.dtype == bf16 else mm_both(d, x)


def compose(earlier, later):
    ce, de, be, fe, le = earlier
    cl, dl, bl, fl, ll = later
    link = jnp.where(le == fl, 1.0, 0.0)
    de = de.astype(f32)
    moved = times(dl, jnp.concatenate([de, be], 1))
    cl = cl * link
    d = cl * de + (link * ce) * dl.astype(f32) - link * moved[:, :DK]
    b = cl * be - link * moved[:, DK:] + bl
    return cl * ce, d, b, fe, ll


def apply_map(parts, link, state):
    c, d, b = parts[:3]
    return link * (c * state - times(d, state) + b)


def inverses(couplings):
    ii, jj = iota((N, N), 0), iota((N, N), 1)
    eye = jnp.where(ii == jj, 1.0, 0.0)
    inside = (ii // 16) == (jj // 16)
    squared = [jnp.where(inside, c, 0.0) for c in couplings]
    inv = [eye - s for s in squared]
    for _ in range(3):
        squared = [mm_both(s, s) for s in squared]
        inv = [x + mm_both(x, s) for x, s in zip(inv, squared)]
    for size in (16, 32, 64):
        ring = ((ii // (2 * size)) == (jj // (2 * size))) & ((ii // size) != (jj // size))
        below = [mm_both(jnp.where(ring, c, 0.0), x) for c, x in zip(couplings, inv)]
        inv = [x - mm_both(x, y) for x, y in zip(inv, below)]
    return inv


def masks(seg_ref):
    ii, jj = iota((N, N), 0), iota((N, N), 1)
    doc_row = jnp.broadcast_to(seg_ref[...].astype(f32), (N, N))
    doc_col = doc_row.T
    return ii, jj, doc_row, doc_col


def local_maps(q_ref, k_ref, v_ref, g_ref, b_ref, seg_ref, own, send, mixes, both, reads, pay):
    core = places()[0]
    ii, jj, doc_row, doc_col = masks(seg_ref)
    same = (doc_row == doc_col) & (ii >= jj)
    strict = same & (ii > jj)
    cont_row = doc_row[0:1] == doc_col[0:1]
    cont_col = doc_col[:, 0:1] == doc_row[:, 0:1]
    last_col = doc_col[:, 0:1] == doc_row[:, N - 1 : N]
    first_doc, last_doc = doc_col[0:1], doc_col[N - 1 : N]
    upper = jnp.where(ii <= jj, 1.0, 0.0).astype(bf16)
    g = g_ref[...]
    beta = b_ref[...]
    g0 = g.astype(bf16)
    g1 = (g - g0.astype(f32)).astype(bf16)
    g2 = (g - g0.astype(f32) - g1.astype(f32)).astype(bf16)
    rows = mm(g0, upper) + mm(g1, upper) + mm(g2, upper)
    heads = g.shape[0]
    groups = heads // 2
    ks = [k_ref[:, i * DK : (i + 1) * DK] for i in range(groups)]
    qs = [q_ref[:, i * DK : (i + 1) * DK] for i in range(groups)]

    def unit(x):
        x = x.astype(f32)
        return lax.rsqrt(jnp.sum(x * x, axis=-1, keepdims=True) + EPS)

    cols = jnp.concatenate([rows, beta, jnp.zeros((N - 2 * heads, N), f32)], 0).T
    cum = cols[:, :heads]
    rk = [unit(k) for k in ks]
    rq = [unit(q) * DK ** (-0.5) for q in qs]
    rk_row = [jnp.broadcast_to(r, (N, N)).T[0:1] for r in rk]
    kts = [k.astype(f32).T.astype(bf16) for k in ks]
    kk = [mm(k, kt) for k, kt in zip(ks, kts)]
    qk = [mm(q, kt) for q, kt in zip(qs, kts)]
    couplings = []
    for h in range(heads):
        i = h // 2
        gap = cum[:, h : h + 1] - rows[h : h + 1]
        mix = jnp.where(same, jnp.exp(jnp.minimum(gap, 0.0)), 0.0) * rk_row[i]
        couplings.append(jnp.where(strict, (cols[:, heads + h : heads + h + 1] * rk[i]) * (mix * kk[i]), 0.0))
        mixes[h] = rq[i] * (mix * qk[i])
    inv = inverses(couplings)
    for h in range(heads):
        i = h // 2
        entry_row = jnp.where(cont_row, jnp.exp(rows[h : h + 1]), 0.0)
        entry_col = jnp.where(cont_col, jnp.exp(cum[:, h : h + 1]), 0.0)
        beta_row = beta[h : h + 1]
        weighted = mm_left(inv[h] * (beta_row * entry_row * rk_row[i]), ks[i])
        pseudo = mm_left(inv[h] * beta_row, v_ref[:, h * DV : (h + 1) * DV])
        pair = jnp.concatenate([weighted, pseudo], 1)
        both[h] = pair
        reads[h] = (entry_col * rq[i]) * qs[i].astype(f32)
        last_gap = jnp.minimum(cum[N - 1 : N, h : h + 1] - cum[:, h : h + 1], 0.0)
        last_keys = jnp.where(last_col, jnp.exp(last_gap), 0.0) * rk[i]
        written = mm_right(kts[i], last_keys * pair)
        pack_wide(pay, (h,), entry_row[:, N - 1 :], written[:, :DK], written[:, DK:], first_doc, last_doc)
    half = heads // 2
    own[...] = pay[pl.ds(core * half, half)]
    send[...] = pay[pl.ds((1 - core) * half, half)]


def local_reads(mixes, both, reads, gate, local, read, silu):
    for h in range(mixes.shape[0]):
        mixed = mm_both(mixes[h], both[h])
        local[h] = mixed[:, DK:]
        read[h] = reads[h] - mixed[:, :DK]
        z = gate[:, h * DV : (h + 1) * DV].astype(f32)
        silu[:, h * DV : (h + 1) * DV] = z / (1.0 + jnp.exp(-z))


def pair_maps(own, got, *refs):
    outs, pair = refs[:4], refs[4]
    core, low, high, _ = places()
    pair[core] = own[...]
    pair[1 - core] = got[...]
    for s in range(4):
        j = low ^ s ^ (2 * high)
        pack(outs[s], *compose(parse_wide(pair[0, j]), parse_wide(pair[1, j])))


def quad_maps(m0, m1, m2, m3, total, prefix, prefix_row, maps):
    low = places()[1]
    for s, m in enumerate((m0, m1, m2, m3)):
        maps[low ^ s] = m[...]
    c, d, b, first, last = parse(maps[0])
    current = (c, d.astype(f32), b, first, last)
    for t in range(3):
        later = parse(maps[t + 1])
        prefix[t, :, :DK] = current[1]
        prefix[t, :, DK:] = current[2]
        row = iota((8, DK), 0)
        link = jnp.where(current[4] == later[3], 1.0, 0.0)
        prefix_row[t] = jnp.where(row == 0, current[0], link)
        current = compose(current, later)
    pack(total, *current)


def row_map(own, got, out, maps):
    high = places()[2]
    maps[high] = own[...]
    maps[1 - high] = got[...]
    pack(out, *compose(parse(maps[0]), parse(maps[1])))


def scan_states(r0, r1, r2, r3, own, got, prefix, prefix_row, o0, o1, o2, o3, maps, halves, final, pay):
    _, low, high, y = places()
    for s, r in enumerate((r0, r1, r2, r3)):
        maps[(y + 4 - s) % 4] = r[...]
    halves[high] = own[...]
    halves[1 - high] = got[...]
    state = jnp.zeros((DK, DV), f32)
    incoming = state
    before = jnp.full((1, DK), -1.0, f32)
    for t in range(4):
        row = parse(maps[t])
        entering = jnp.where(before == row[3], 1.0, 0.0) * state
        incoming = jnp.where(y == t, entering, incoming)
        state = apply_map(row, 1.0, entering)
        before = row[4]
    final[...] = state
    first_half = parse(halves[0])
    link = jnp.where(first_half[4] == parse(halves[1])[3], 1.0, 0.0)
    start = jnp.where(high == 1, apply_map(first_half, link, incoming), incoming)
    for t in range(4):
        here = start
        if t:
            c, link = prefix_row[t - 1, 0:1], prefix_row[t - 1, 1:2]
            here = apply_map((c, prefix[t - 1, :, :DK], prefix[t - 1, :, DK:]), link, start)
        pay[t, :DK] = here.astype(bf16)
        rows = final[pl.ds(4 * (y * 8 + high * 4 + t), 4)]
        hi = rows.astype(bf16).astype(f32)
        pay[t, DK:] = jnp.concatenate([hi, rows - hi, jnp.zeros((8, DV), f32)], 0).astype(bf16)
    for s, o in enumerate((o0, o1, o2, o3)):
        o[...] = pay[low ^ s]


def pair_states(s0, s1, s2, s3, own, got, own_out, send_out, pair, states, starts):
    core, low, high, _ = places()
    pair[core] = own[...]
    pair[1 - core] = got[...]
    for s, ref in enumerate((s0, s1, s2, s3)):
        starts[low ^ s ^ (2 * high)] = ref[...]
    for j in range(own.shape[0]):
        c, d, b, first, last = parse_wide(pair[0, j])
        link = jnp.where(last == parse_wide(pair[1, j])[3], 1.0, 0.0)
        start = starts[j, :DK]
        states[0, j, :DK] = start.astype(f32)
        states[1, j, :DK] = link * (c * start.astype(f32) - mm_left(d, start) + b)
        rows = starts[j, DK:].astype(f32)
        rows = jnp.concatenate([rows[:4] + rows[4:8], rows[8:12]], 0)
        states[0, j, DK:] = rows
        states[1, j, DK:] = rows
    own_out[...] = states[core]
    send_out[...] = states[1 - core]


def project(own, got, local, read, silu, w, acc, o1, o2, o3, tail, states, normed, total):
    core = places()[0]
    x = lax.axis_index("head")
    half = own.shape[0]
    states[pl.ds(core * half, half)] = own[...]
    states[pl.ds((1 - core) * half, half)] = got[...]
    finals = []
    for h in range(2 * half):
        attention = local[h] + mm_both(read[h], states[h, :DK])
        mean_square = jnp.mean(attention * attention, axis=-1, keepdims=True)
        gated = attention * lax.rsqrt(mean_square + EPS) * silu[:, h * DV : (h + 1) * DV]
        normed[:, h * DV : (h + 1) * DV] = gated.astype(bf16)
        rows = states[h, DK:]
        finals.append(jnp.where(core == 0, rows[0:2], rows[2:4]))
    finals = jnp.concatenate(finals, 0)
    hi = finals.astype(bf16).astype(f32)
    tail[...] = jnp.concatenate([hi, finals - hi], 0).astype(bf16)
    total[...] = mm(normed[...], w[...])
    acc[...] = total[pl.ds(x * 32, 32)]
    width = total.shape[1]
    for s, o in enumerate((o1, o2, o3)):
        o[:, :width] = total[pl.ds((x ^ (s + 1)) * 32, 32)].astype(bf16)
        o[:, width:] = tail[...]


def finish(order, acc, r1, r2, r3, tail, out, decode, final):
    x = lax.axis_index("head")
    total = acc[...]
    width = total.shape[1]
    for r in (r1, r2, r3):
        total = total + r[:, :width].astype(f32)
    out[...] = total.astype(bf16)
    slots = decode.shape[0]
    for s, block in enumerate((tail[...], r1[:, width:], r2[:, width:], r3[:, width:])):
        block = block.astype(f32)
        rows = block[:16] + block[16:]
        for h in range(slots):
            line = jnp.concatenate([rows[2 * h : 2 * h + 1], rows[2 * h + 1 : 2 * h + 2]], 1)
            final[pl.ds((x ^ s) * slots + h, 1)] = line
    for i in range(slots):
        decode[i : i + 1] = final[pl.ds(order[x * slots + i], 1)]


def shape(dims, dtype=bf16):
    return pltpu.VMEM(dims, dtype)


def call(kernel, outs, scratch, *args, name, smem=0, hbm=(), flops=None):
    specs = [pl.BlockSpec(memory_space=pltpu.SMEM)] * smem
    specs += [pl.BlockSpec(memory_space=pltpu.VMEM)] * (len(args) - smem)
    args = [
        a if i < smem or i in hbm else pltpu.with_memory_space_constraint(a, pltpu.VMEM)
        for i, a in enumerate(args)
    ]
    cost = None if flops is None else pl.CostEstimate(flops=flops, transcendentals=0, bytes_accessed=0)
    return pl.pallas_call(
        kernel,
        out_shape=outs,
        scratch_shapes=scratch,
        name=name,
        in_specs=specs,
        cost_estimate=cost,
        compiler_params=pltpu.CompilerParams(vmem_limit_bytes=24 * 2**20),
    )(*args)


def xor_peers(count, bit):
    return [(i, i ^ bit) for i in range(count)]


def per_device(
    queries, keys, values, out_gate, log_decay, write_strength, segment_ids, head_order, out_weight
):
    heads = values.shape[1] // DV
    half = heads // 2
    peers = lax.axis_size("ctx")
    model = out_weight.shape[1]
    wide = (N + 8, 256)
    block = (ROWS, 256)
    block3 = (ROWS, 384)
    seg = segment_ids.reshape(1, N)
    own, send, mixes, both, reads = call(
        local_maps,
        [shape((half,) + wide, f32)] * 2
        + [shape((heads, N, N), f32), shape((heads, N, 256), f32), shape((heads, N, DK), f32)],
        [pltpu.VMEM((heads,) + wide, f32)],
        queries, keys, values, log_decay.T, write_strength.T, seg,
        name="local_maps",
    )
    got = lax.ppermute(send, "ctx", xor_peers(peers, 1))
    m0, m1, m2, m3 = call(
        pair_maps,
        [shape(block)] * 4,
        [pltpu.VMEM((2, half) + wide, f32)],
        own, got,
        name="pair_maps",
    )
    m1, m2, m3 = [lax.ppermute(m, "ctx", xor_peers(peers, 2 * s)) for s, m in ((1, m1), (2, m2), (3, m3))]
    local, read, silu = call(
        local_reads,
        [shape((heads, N, DV), f32), shape((heads, N, DK), f32), shape((N, heads * DV), f32)],
        [],
        mixes, both, reads, out_gate,
        name="local_reads",
        flops=2 * 10**9,
    )
    total, prefix, prefix_row = call(
        quad_maps,
        [shape(block3), shape((3, DK, 256), f32), shape((3, 8, DK), f32)],
        [pltpu.VMEM((4,) + block, bf16)],
        m0, m1, m2, m3,
        name="quad_maps",
    )
    total_got = lax.ppermute(total, "ctx", xor_peers(peers, 12))
    r0 = call(
        row_map,
        shape(block3),
        [pltpu.VMEM((2,) + block3, bf16)],
        total, total_got,
        name="row_map",
    )
    r1, r2, r3 = [
        lax.ppermute(r0, "ctx", [(i, (i + 16 * s) % peers) for i in range(peers)]) for s in (1, 2, 3)
    ]
    s0, s1, s2, s3 = call(
        scan_states,
        [shape((ROWS, DV))] * 4,
        [
            pltpu.VMEM((4,) + block3, bf16),
            pltpu.VMEM((2,) + block3, bf16),
            pltpu.VMEM((DK, DV), f32),
            pltpu.VMEM((4, ROWS, DV), bf16),
        ],
        r0, r1, r2, r3, total, total_got, prefix, prefix_row,
        name="scan_states",
    )
    s1, s2, s3 = [lax.ppermute(m, "ctx", xor_peers(peers, 2 * s)) for s, m in ((1, s1), (2, s2), (3, s3))]
    own_state, send_state = call(
        pair_states,
        [shape((half, N + 8, DV), f32)] * 2,
        [
            pltpu.VMEM((2, half) + wide, f32),
            pltpu.VMEM((2, half, N + 8, DV), f32),
            pltpu.VMEM((half, ROWS, DV), bf16),
        ],
        s0, s1, s2, s3, own, got,
        name="pair_states",
    )
    got_state = lax.ppermute(send_state, "ctx", xor_peers(peers, 1))
    acc, o1, o2, o3, tail = call(
        project,
        [shape((32, model), f32)] + [shape((32, model + DV))] * 3 + [shape((32, DV))],
        [
            pltpu.VMEM((heads, N + 8, DV), f32),
            pltpu.VMEM((N, heads * DV), bf16),
            pltpu.VMEM((N, model), f32),
        ],
        own_state, got_state, local, read, silu, out_weight,
        name="project",
    )
    o1, o2, o3 = [lax.ppermute(o, "head", xor_peers(4, s)) for s, o in ((1, o1), (2, o2), (3, o3))]
    return call(
        finish,
        [jax.ShapeDtypeStruct((32, model), bf16), jax.ShapeDtypeStruct((heads, 256), f32)],
        [pltpu.VMEM((4 * heads, 256), f32)],
        head_order, acc, o1, o2, o3, tail,
        name="finish",
        smem=1,
    )


def solution(mesh):
    in_specs = (
        P("ctx", "head"),
        P("ctx", "head"),
        P("ctx", "head"),
        P("ctx", "head"),
        P("ctx", "head"),
        P("ctx", "head"),
        P("ctx"),
        P(),
        P("head", None),
    )
    out_specs = (P(("ctx", "head"), None), P("head", "ctx"))

    def run(*args):
        return tuple(per_device(*args))

    return jax.shard_map(run, mesh=mesh, in_specs=in_specs, out_specs=out_specs, check_vma=False)
```

```python
import jax
import jax.numpy as jnp
from jax import lax
from jax.experimental import pallas as pl
from jax.experimental.pallas import tpu as pltpu
from jax.sharding import PartitionSpec as P


f32 = jnp.float32
bf16 = jnp.bfloat16
DK = 128
DV = 128
N = 128
ROWS = N + 16
EPS = 1e-06


def mm(a, b):
    return jnp.dot(a, b, preferred_element_type=f32)


def split(x):
    hi = x.astype(bf16)
    return hi, (x - hi.astype(f32)).astype(bf16)


def mm_left(a, b):
    hi, lo = split(a)
    return mm(jnp.concatenate([hi, lo], 1), jnp.concatenate([b, b], 0))


def mm_right(a, b):
    hi, lo = split(b)
    return mm(jnp.concatenate([a, a], 1), jnp.concatenate([hi, lo], 0))


def mm_both(a, b):
    ah, al = split(a)
    bh, bl = split(b)
    return mm(jnp.concatenate([ah, al], 1), jnp.concatenate([bh, bh], 0)) + mm(ah, bl)


def iota(shape, axis):
    return lax.broadcasted_iota(jnp.int32, shape, axis)


def places():
    ctx = lax.axis_index("ctx")
    return ctx % 2, (ctx // 2) % 4, (ctx // 8) % 2, ctx // 16


def lines(shape, values):
    row = iota(shape, 0)
    out = jnp.zeros(shape, f32)
    for i, value in enumerate(values):
        out = jnp.where(row == i, jnp.broadcast_to(value[:, :1], shape), out)
    return out


def pack_wide(ref, at, c, d, b, first, last):
    ref[at + (pl.ds(0, N), pl.ds(0, DK))] = d
    ref[at + (pl.ds(0, N), pl.ds(DK, DV))] = b
    ref[at + (pl.ds(N, 8), slice(None))] = lines((8, 256), (c, first, last))


def parse_wide(block):
    tail = block[N:, :DK]
    return tail[0:1], block[:N, :DK], block[:N, DK:], tail[1:2], tail[2:3]


def pack(ref, c, d, b, first, last):
    c0 = c.astype(bf16).astype(f32)
    c1 = (c - c0).astype(bf16).astype(f32)
    ref[:N, :DK] = d.astype(bf16)
    hi = b.astype(bf16)
    ref[:N, DK : 2 * DK] = hi
    if ref.shape[1] > 2 * DK:
        ref[:N, 2 * DK :] = (b - hi.astype(f32)).astype(bf16)
    ref[N:] = lines((16, ref.shape[1]), (c0, c1, c - c0 - c1, first, last)).astype(bf16)


def parse(block):
    tail = block[N:, :DK].astype(f32)
    c = tail[0:1] + tail[1:2] + tail[2:3]
    b = block[:N, DK : 2 * DK].astype(f32)
    if block.shape[1] > 2 * DK:
        b = b + block[:N, 2 * DK :].astype(f32)
    return c, block[:N, :DK], b, tail[3:4], tail[4:5]


def times(d, x):
    return mm_right(d, x) if d.dtype == bf16 else mm_both(d, x)


def compose(earlier, later):
    ce, de, be, fe, le = earlier
    cl, dl, bl, fl, ll = later
    link = jnp.where(le == fl, 1.0, 0.0)
    de = de.astype(f32)
    moved = times(dl, jnp.concatenate([de, be], 1))
    cl = cl * link
    d = cl * de + (link * ce) * dl.astype(f32) - link * moved[:, :DK]
    b = cl * be - link * moved[:, DK:] + bl
    return cl * ce, d, b, fe, ll


def apply_map(parts, link, state):
    c, d, b = parts[:3]
    return link * (c * state - times(d, state) + b)


def inverses(couplings):
    ii, jj = iota((N, N), 0), iota((N, N), 1)
    eye = jnp.where(ii == jj, 1.0, 0.0)
    inside = (ii // 16) == (jj // 16)
    squared = [jnp.where(inside, c, 0.0) for c in couplings]
    inv = [eye - s for s in squared]
    for _ in range(3):
        squared = [mm_both(s, s) for s in squared]
        inv = [x + mm_both(x, s) for x, s in zip(inv, squared)]
    for size in (16, 32, 64):
        ring = ((ii // (2 * size)) == (jj // (2 * size))) & ((ii // size) != (jj // size))
        below = [mm_both(jnp.where(ring, c, 0.0), x) for c, x in zip(couplings, inv)]
        inv = [x - mm_both(x, y) for x, y in zip(inv, below)]
    return inv


def local_maps(heads, groups, q_ref, k_ref, v_ref, g, beta, seg_ref, out, mixes, both, reads):
    ii, jj = iota((N, N), 0), iota((N, N), 1)
    doc_row = jnp.broadcast_to(seg_ref[...].astype(f32), (N, N))
    doc_col = doc_row.T
    same = (doc_row == doc_col) & (ii >= jj)
    strict = same & (ii > jj)
    cont_row = doc_row[0:1] == doc_col[0:1]
    cont_col = doc_col[:, 0:1] == doc_row[:, 0:1]
    last_col = doc_col[:, 0:1] == doc_row[:, N - 1 : N]
    first_doc, last_doc = doc_col[0:1], doc_col[N - 1 : N]
    upper = jnp.where(ii <= jj, 1.0, 0.0).astype(bf16)
    count = g.shape[0]
    g = jnp.concatenate([g, jnp.zeros((8 - count, N), f32)], 0)
    g0 = g.astype(bf16)
    g1 = (g - g0.astype(f32)).astype(bf16)
    g2 = (g - g0.astype(f32) - g1.astype(f32)).astype(bf16)
    rows = mm(g0, upper) + mm(g1, upper) + mm(g2, upper)
    ks = [k_ref[:, pl.ds(pl.multiple_of((groups + i) * DK, DK), DK)] for i in range(count // 2)]
    qs = [q_ref[:, pl.ds(pl.multiple_of((groups + i) * DK, DK), DK)] for i in range(count // 2)]

    def unit(x):
        x = x.astype(f32)
        return lax.rsqrt(jnp.sum(x * x, axis=-1, keepdims=True) + EPS)

    cols = jnp.concatenate([rows, beta, jnp.zeros((N - 8 - count, N), f32)], 0).T
    cum = cols[:, :count]
    rk = [unit(k) for k in ks]
    rq = [unit(q) * DK ** (-0.5) for q in qs]
    rk_row = [jnp.broadcast_to(r, (N, N)).T[0:1] for r in rk]
    kts = [k.astype(f32).T.astype(bf16) for k in ks]
    kk = [mm(k, kt) for k, kt in zip(ks, kts)]
    qk = [mm(q, kt) for q, kt in zip(qs, kts)]
    couplings = []
    for h in range(count):
        i = h // 2
        gap = cum[:, h : h + 1] - rows[h : h + 1]
        mix = jnp.where(same, jnp.exp(jnp.minimum(gap, 0.0)), 0.0) * rk_row[i]
        couplings.append(jnp.where(strict, (cols[:, 8 + h : 9 + h] * rk[i]) * (mix * kk[i]), 0.0))
        mixes[h] = rq[i] * (mix * qk[i])
    inv = inverses(couplings)
    for h in range(count):
        i = h // 2
        entry_row = jnp.where(cont_row, jnp.exp(rows[h : h + 1]), 0.0)
        entry_col = jnp.where(cont_col, jnp.exp(cum[:, h : h + 1]), 0.0)
        beta_row = beta[h : h + 1]
        weighted = mm_left(inv[h] * (beta_row * entry_row * rk_row[i]), ks[i])
        pseudo = mm_left(inv[h] * beta_row, v_ref[:, pl.ds(pl.multiple_of((heads + h) * DV, DV), DV)])
        pair = jnp.concatenate([weighted, pseudo], 1)
        both[h] = pair
        reads[h] = (entry_col * rq[i]) * qs[i].astype(f32)
        last_gap = jnp.minimum(cum[N - 1 : N, h : h + 1] - cum[:, h : h + 1], 0.0)
        last_keys = jnp.where(last_col, jnp.exp(last_gap), 0.0) * rk[i]
        written = mm_right(kts[i], last_keys * pair)
        pack_wide(out, (h,), entry_row[:, N - 1 :], written[:, :DK], written[:, DK:], first_doc, last_doc)


def send_maps(q, k, v, g, b, seg, out, mixes, both, reads, q_in, k_in, v_in, g_in, b_in, seg_in, sems):
    moves = [
        pltpu.make_async_copy(src, dst, sems.at[i])
        for i, (src, dst) in enumerate(
            ((seg, seg_in), (g, g_in), (b, b_in), (k, k_in), (q, q_in), (v, v_in))
        )
    ]
    for move in moves:
        move.start()
    for move in moves:
        move.wait()
    half = out.shape[0]
    heads = (1 - places()[0]) * half
    local_maps(
        heads, heads // 2, q_in, k_in, v_in, g_in[pl.ds(heads, half)], b_in[pl.ds(heads, half)], seg_in,
        out, mixes, both, reads,
    )


def own_maps(q, k, v, g, b, seg, out, mixes, both, reads):
    half = out.shape[0]
    heads = places()[0] * half
    local_maps(
        heads, heads // 2, q, k, v, g[pl.ds(heads, half)], b[pl.ds(heads, half)], seg,
        out, mixes, both, reads,
    )


def local_reads(mixes0, both0, reads0, mixes1, both1, reads1, gate, local, read, silu):
    core = places()[0]
    half = mixes0.shape[0]
    width = half * DV
    for part, (mixes, both, reads) in enumerate(((mixes0, both0, reads0), (mixes1, both1, reads1))):
        for h in range(half):
            mixed = mm_both(mixes[h], both[h])
            local[part * half + h] = mixed[:, DK:]
            read[part * half + h] = reads[h] - mixed[:, :DK]
        first = pl.multiple_of((core ^ part) * width, width)
        z = gate[:, pl.ds(first, width)].astype(f32)
        silu[:, part * width : (part + 1) * width] = z / (1.0 + jnp.exp(-z))


def pair_maps(own, got, *refs):
    outs, pair = refs[:4], refs[4]
    core, low, high, _ = places()
    pair[core] = own[...]
    pair[1 - core] = got[...]
    for s in range(4):
        j = low ^ s ^ (2 * high)
        pack(outs[s], *compose(parse_wide(pair[0, j]), parse_wide(pair[1, j])))


def quad_maps(m0, m1, m2, m3, total, prefix, prefix_row, maps):
    low = places()[1]
    for s, m in enumerate((m0, m1, m2, m3)):
        maps[low ^ s] = m[...]
    c, d, b, first, last = parse(maps[0])
    current = (c, d.astype(f32), b, first, last)
    for t in range(3):
        later = parse(maps[t + 1])
        prefix[t, :, :DK] = current[1]
        prefix[t, :, DK:] = current[2]
        row = iota((8, DK), 0)
        link = jnp.where(current[4] == later[3], 1.0, 0.0)
        prefix_row[t] = jnp.where(row == 0, current[0], link)
        current = compose(current, later)
    pack(total, *current)


def row_map(own, got, out, maps):
    high = places()[2]
    maps[high] = own[...]
    maps[1 - high] = got[...]
    pack(out, *compose(parse(maps[0]), parse(maps[1])))


def scan_states(r0, r1, r2, r3, own, got, prefix, prefix_row, o0, o1, o2, o3, maps, halves, final, pay):
    _, low, high, y = places()
    for s, r in enumerate((r0, r1, r2, r3)):
        maps[(y + 4 - s) % 4] = r[...]
    halves[high] = own[...]
    halves[1 - high] = got[...]
    state = jnp.zeros((DK, DV), f32)
    incoming = state
    before = jnp.full((1, DK), -1.0, f32)
    for t in range(4):
        row = parse(maps[t])
        entering = jnp.where(before == row[3], 1.0, 0.0) * state
        incoming = jnp.where(y == t, entering, incoming)
        state = apply_map(row, 1.0, entering)
        before = row[4]
    final[...] = state
    first_half = parse(halves[0])
    link = jnp.where(first_half[4] == parse(halves[1])[3], 1.0, 0.0)
    start = jnp.where(high == 1, apply_map(first_half, link, incoming), incoming)
    for t in range(4):
        here = start
        if t:
            c, link = prefix_row[t - 1, 0:1], prefix_row[t - 1, 1:2]
            here = apply_map((c, prefix[t - 1, :, :DK], prefix[t - 1, :, DK:]), link, start)
        pay[t, :DK] = here.astype(bf16)
        rows = final[pl.ds(4 * (y * 8 + high * 4 + t), 4)]
        hi = rows.astype(bf16).astype(f32)
        pay[t, DK:] = jnp.concatenate([hi, rows - hi, jnp.zeros((8, DV), f32)], 0).astype(bf16)
    for s, o in enumerate((o0, o1, o2, o3)):
        o[...] = pay[low ^ s]


def pair_states(s0, s1, s2, s3, own, got, own_out, send_out, pair, states, starts):
    core, low, high, _ = places()
    pair[core] = own[...]
    pair[1 - core] = got[...]
    for s, ref in enumerate((s0, s1, s2, s3)):
        starts[low ^ s ^ (2 * high)] = ref[...]
    for j in range(own.shape[0]):
        c, d, b, _, last = parse_wide(pair[0, j])
        link = jnp.where(last == parse_wide(pair[1, j])[3], 1.0, 0.0)
        start = starts[j, :DK]
        states[0, j, :DK] = start.astype(f32)
        states[1, j, :DK] = link * (c * start.astype(f32) - mm_left(d, start) + b)
        rows = starts[j, DK:].astype(f32)
        rows = jnp.concatenate([rows[:4] + rows[4:8], rows[8:12]], 0)
        states[0, j, DK:] = rows
        states[1, j, DK:] = rows
    own_out[...] = states[core]
    send_out[...] = states[1 - core]


def project(own, got, local, read, silu, w, acc, o1, o2, o3, tail, normed, total, lasts):
    core = places()[0]
    x = lax.axis_index("head")
    half = own.shape[0]
    width = half * DV
    for part, states in enumerate((own, got)):
        gated = []
        for h in range(half):
            at = part * half + h
            attention = local[at] + mm_both(read[at], states[h, :DK])
            mean_square = jnp.mean(attention * attention, axis=-1, keepdims=True)
            weight = lax.rsqrt(mean_square + EPS) * silu[:, at * DV : (at + 1) * DV]
            gated.append((attention * weight).astype(bf16))
            lasts[(core ^ part) * half + h] = states[h, DK:]
        first = pl.multiple_of((core ^ part) * width, width)
        normed[:, pl.ds(first, width)] = jnp.concatenate(gated, 1)
    finals = []
    for h in range(2 * half):
        rows = lasts[h]
        finals.append(jnp.where(core == 0, rows[0:2], rows[2:4]))
    finals = jnp.concatenate(finals, 0)
    hi = finals.astype(bf16).astype(f32)
    tail[...] = jnp.concatenate([hi, finals - hi], 0).astype(bf16)
    total[...] = mm(normed[...], w[...])
    acc[...] = total[pl.ds(x * 32, 32)]
    width = total.shape[1]
    for s, o in enumerate((o1, o2, o3)):
        o[:, :width] = total[pl.ds((x ^ (s + 1)) * 32, 32)].astype(bf16)
        o[:, width:] = tail[...]


def finish(order, acc, r1, r2, r3, tail, out, decode, final):
    x = lax.axis_index("head")
    total = acc[...]
    width = total.shape[1]
    for r in (r1, r2, r3):
        total = total + r[:, :width].astype(f32)
    out[...] = total.astype(bf16)
    slots = decode.shape[0]
    for s, block in enumerate((tail[...], r1[:, width:], r2[:, width:], r3[:, width:])):
        block = block.astype(f32)
        rows = block[:16] + block[16:]
        for h in range(slots):
            line = jnp.concatenate([rows[2 * h : 2 * h + 1], rows[2 * h + 1 : 2 * h + 2]], 1)
            final[pl.ds((x ^ s) * slots + h, 1)] = line
    for i in range(slots):
        decode[i : i + 1] = final[pl.ds(order[x * slots + i], 1)]


def shape(dims, dtype=bf16):
    return pltpu.VMEM(dims, dtype)


def call(kernel, outs, scratch, *args, smem=0, hbm=(), flops=None):
    specs = [pl.BlockSpec(memory_space=pltpu.SMEM)] * smem
    specs += [
        pl.BlockSpec(memory_space=pltpu.HBM if i in hbm else pltpu.VMEM) for i in range(smem, len(args))
    ]
    args = [
        a if i < smem else pltpu.with_memory_space_constraint(a, pltpu.HBM if i in hbm else pltpu.VMEM)
        for i, a in enumerate(args)
    ]
    cost = None if flops is None else pl.CostEstimate(flops=flops, transcendentals=0, bytes_accessed=0)
    return pl.pallas_call(
        kernel,
        out_shape=outs,
        scratch_shapes=scratch,
        in_specs=specs,
        cost_estimate=cost,
        compiler_params=pltpu.CompilerParams(vmem_limit_bytes=24 * 2**20),
    )(*args)


def move(x, axis, pairs):
    return lax.ppermute(x, axis, pairs)


def xor_peers(count, bit):
    return [(i, i ^ bit) for i in range(count)]


def per_device(
    queries, keys, values, out_gate, log_decay, write_strength, segment_ids, head_order, out_weight
):
    heads = values.shape[1] // DV
    half = heads // 2
    peers = lax.axis_size("ctx")
    model = out_weight.shape[1]
    wide = (N + 8, 256)
    block = (ROWS, 256)
    block3 = (ROWS, 384)
    seg = segment_ids.reshape(1, N)
    maps = [
        shape((half,) + wide, f32),
        shape((half, N, N), f32),
        shape((half, N, 256), f32),
        shape((half, N, DK), f32),
    ]
    inputs = (queries, keys, values, log_decay.T, write_strength.T, seg)
    send, mixes1, both1, reads1, *held = call(
        send_maps,
        maps + [shape(a.shape, a.dtype) for a in inputs],
        [pltpu.SemaphoreType.DMA((6,))],
        *inputs,
        hbm=range(6),
    )
    got = lax.ppermute(send, "ctx", xor_peers(peers, 1))
    own, mixes0, both0, reads0 = call(own_maps, maps, [], *held, flops=10**9)
    m0, m1, m2, m3 = call(
        pair_maps,
        [shape(block)] * 4,
        [pltpu.VMEM((2, half) + wide, f32)],
        own, got,
    )
    m1, m2, m3 = [move(m, "ctx", xor_peers(peers, 2 * s)) for s, m in ((1, m1), (2, m2), (3, m3))]
    local, read, silu = call(
        local_reads,
        [shape((heads, N, DV), f32), shape((heads, N, DK), f32), shape((N, heads * DV), f32)],
        [],
        mixes0, both0, reads0, mixes1, both1, reads1, out_gate,
        flops=2 * 10**9,
    )
    total, prefix, prefix_row = call(
        quad_maps,
        [shape(block3), shape((3, DK, 256), f32), shape((3, 8, DK), f32)],
        [pltpu.VMEM((4,) + block, bf16)],
        m0, m1, m2, m3,
    )
    total_got = lax.ppermute(total, "ctx", xor_peers(peers, 12))
    r0 = call(
        row_map,
        shape(block3),
        [pltpu.VMEM((2,) + block3, bf16)],
        total, total_got,
    )
    rows = [[(i, (i + 16 * s) % peers) for i in range(peers)] for s in (1, 2, 3)]
    rows[2] = [(i, i - 16) for i in range(peers // 2, peers)]
    r1, r2, r3 = [move(r0, "ctx", pairs) for pairs in rows]
    s0, s1, s2, s3 = call(
        scan_states,
        [shape((ROWS, DV))] * 4,
        [
            pltpu.VMEM((4,) + block3, bf16),
            pltpu.VMEM((2,) + block3, bf16),
            pltpu.VMEM((DK, DV), f32),
            pltpu.VMEM((4, ROWS, DV), bf16),
        ],
        r0, r1, r2, r3, total, total_got, prefix, prefix_row,
    )
    s1, s2, s3 = [move(m, "ctx", xor_peers(peers, 2 * s)) for s, m in ((1, s1), (2, s2), (3, s3))]
    own_state, send_state = call(
        pair_states,
        [shape((half, N + 8, DV), f32)] * 2,
        [
            pltpu.VMEM((2, half) + wide, f32),
            pltpu.VMEM((2, half, N + 8, DV), f32),
            pltpu.VMEM((half, ROWS, DV), bf16),
        ],
        s0, s1, s2, s3, own, got,
    )
    got_state = lax.ppermute(send_state, "ctx", xor_peers(peers, 1))
    acc, o1, o2, o3, tail = call(
        project,
        [shape((32, model), f32)] + [shape((32, model + DV))] * 3 + [shape((32, DV))],
        [
            pltpu.VMEM((N, heads * DV), bf16),
            pltpu.VMEM((N, model), f32),
            pltpu.VMEM((heads, 8, DV), f32),
        ],
        own_state, got_state, local, read, silu, out_weight,
    )
    o1, o2, o3 = [move(o, "head", xor_peers(4, s)) for s, o in ((1, o1), (2, o2), (3, o3))]
    return call(
        finish,
        [jax.ShapeDtypeStruct((32, model), bf16), jax.ShapeDtypeStruct((heads, 256), f32)],
        [pltpu.VMEM((4 * heads, 256), f32)],
        head_order, acc, o1, o2, o3, tail,
        smem=1,
    )


def solution(mesh):
    in_specs = (
        P("ctx", "head"),
        P("ctx", "head"),
        P("ctx", "head"),
        P("ctx", "head"),
        P("ctx", "head"),
        P("ctx", "head"),
        P("ctx"),
        P(),
        P("head", None),
    )
    out_specs = (P(("ctx", "head"), None), P("head", "ctx"))

    def run(*args):
        return tuple(per_device(*args))

    return jax.shard_map(run, mesh=mesh, in_specs=in_specs, out_specs=out_specs, check_vma=False)
```

```python
import jax
import jax.numpy as jnp
from jax import lax
from jax.experimental import pallas as pl
from jax.experimental.pallas import tpu as pltpu
from jax.sharding import PartitionSpec as P


f32 = jnp.float32
bf16 = jnp.bfloat16
DK = 128
DV = 128
N = 128
ROWS = N + 16
EPS = 1e-06


def mm(a, b):
    return jnp.dot(a, b, preferred_element_type=f32)


def split(x):
    hi = x.astype(bf16)
    return hi, (x - hi.astype(f32)).astype(bf16)


def mm_left(a, b):
    hi, lo = split(a)
    return mm(jnp.concatenate([hi, lo], 1), jnp.concatenate([b, b], 0))


def mm_right(a, b):
    hi, lo = split(b)
    return mm(jnp.concatenate([a, a], 1), jnp.concatenate([hi, lo], 0))


def mm_both(a, b):
    ah, al = split(a)
    bh, bl = split(b)
    return mm(jnp.concatenate([ah, al], 1), jnp.concatenate([bh, bh], 0)) + mm(ah, bl)


def iota(shape, axis):
    return lax.broadcasted_iota(jnp.int32, shape, axis)


def places():
    ctx = lax.axis_index("ctx")
    return ctx % 2, (ctx // 2) % 4, (ctx // 8) % 2, ctx // 16


def lines(shape, values):
    row = iota(shape, 0)
    out = jnp.zeros(shape, f32)
    for i, value in enumerate(values):
        out = jnp.where(row == i, jnp.broadcast_to(value[:, :1], shape), out)
    return out


def pack_wide(ref, at, c, d, b, first, last):
    ref[at + (pl.ds(0, N), pl.ds(0, DK))] = d
    ref[at + (pl.ds(0, N), pl.ds(DK, DV))] = b
    ref[at + (pl.ds(N, 8), slice(None))] = lines((8, 256), (c, first, last))


def parse_wide(block):
    tail = block[N:, :DK]
    return tail[0:1], block[:N, :DK], block[:N, DK:], tail[1:2], tail[2:3]


def pack(ref, c, d, b, first, last):
    c0 = c.astype(bf16).astype(f32)
    c1 = (c - c0).astype(bf16).astype(f32)
    ref[:N, :DK] = d.astype(bf16)
    hi = b.astype(bf16)
    ref[:N, DK : 2 * DK] = hi
    if ref.shape[1] > 2 * DK:
        ref[:N, 2 * DK :] = (b - hi.astype(f32)).astype(bf16)
    ref[N:] = lines((16, ref.shape[1]), (c0, c1, c - c0 - c1, first, last)).astype(bf16)


def parse(block):
    tail = block[N:, :DK].astype(f32)
    c = tail[0:1] + tail[1:2] + tail[2:3]
    b = block[:N, DK : 2 * DK].astype(f32)
    if block.shape[1] > 2 * DK:
        b = b + block[:N, 2 * DK :].astype(f32)
    return c, block[:N, :DK], b, tail[3:4], tail[4:5]


def times(d, x):
    return mm_right(d, x) if d.dtype == bf16 else mm_both(d, x)


def compose(earlier, later):
    ce, de, be, fe, le = earlier
    cl, dl, bl, fl, ll = later
    link = jnp.where(le == fl, 1.0, 0.0)
    de = de.astype(f32)
    moved = times(dl, jnp.concatenate([de, be], 1))
    cl = cl * link
    d = cl * de + (link * ce) * dl.astype(f32) - link * moved[:, :DK]
    b = cl * be - link * moved[:, DK:] + bl
    return cl * ce, d, b, fe, ll


def apply_map(parts, link, state):
    c, d, b = parts[:3]
    return link * (c * state - times(d, state) + b)


def inverses(couplings):
    ii, jj = iota((N, N), 0), iota((N, N), 1)
    eye = jnp.where(ii == jj, 1.0, 0.0)
    inside = (ii // 16) == (jj // 16)
    squared = [jnp.where(inside, c, 0.0) for c in couplings]
    inv = [eye - s for s in squared]
    for _ in range(3):
        squared = [mm_both(s, s) for s in squared]
        inv = [x + mm_both(x, s) for x, s in zip(inv, squared)]
    for size in (16, 32, 64):
        odd = range(size, N, 2 * size)
        sibling = (ii // (2 * size)) == (jj // (2 * size))
        ring = sibling & ((ii // size) != (jj // size))

        def take(x):
            return jnp.concatenate([x[r : r + size] for r in odd], 0)

        def spread(x):
            gap = jnp.zeros((size, N), f32)
            return jnp.concatenate([y for i in range(len(odd)) for y in (gap, x[i * size : (i + 1) * size])], 0)

        below = [mm_both(take(jnp.where(ring, c, 0.0)), x) for c, x in zip(couplings, inv)]
        inv = [x - spread(mm_both(take(x), spread(y))) for x, y in zip(inv, below)]
    return inv


def local_maps(heads, q_ref, k_ref, v_ref, g_ref, b_ref, seg_ref, out, mixes, both, reads, waits=None):
    q_wait, v_wait = waits or (None, None)
    groups = heads // 2
    ii, jj = iota((N, N), 0), iota((N, N), 1)
    doc_row = jnp.broadcast_to(seg_ref[...].astype(f32), (N, N))
    doc_col = doc_row.T
    same = (doc_row == doc_col) & (ii >= jj)
    strict = same & (ii > jj)
    cont_row = doc_row[0:1] == doc_col[0:1]
    cont_col = doc_col[:, 0:1] == doc_row[:, 0:1]
    last_col = doc_col[:, 0:1] == doc_row[:, N - 1 : N]
    first_doc, last_doc = doc_col[0:1], doc_col[N - 1 : N]
    upper = jnp.where(ii <= jj, 1.0, 0.0).astype(bf16)
    count = out.shape[0]
    g = g_ref[pl.ds(heads, count)]
    beta = b_ref[pl.ds(heads, count)]
    g = jnp.concatenate([g, jnp.zeros((8 - count, N), f32)], 0)
    g0 = g.astype(bf16)
    g1 = (g - g0.astype(f32)).astype(bf16)
    g2 = (g - g0.astype(f32) - g1.astype(f32)).astype(bf16)
    rows = mm(g0, upper) + mm(g1, upper) + mm(g2, upper)
    ks = [k_ref[:, pl.ds(pl.multiple_of((groups + i) * DK, DK), DK)] for i in range(count // 2)]

    def unit(x):
        x = x.astype(f32)
        return lax.rsqrt(jnp.sum(x * x, axis=-1, keepdims=True) + EPS)

    cols = jnp.concatenate([rows, beta, jnp.zeros((N - 8 - count, N), f32)], 0).T
    cum = cols[:, :count]
    rk = [unit(k) for k in ks]
    rk_row = [jnp.broadcast_to(r, (N, N)).T[0:1] for r in rk]
    kts = [k.astype(f32).T.astype(bf16) for k in ks]
    kk = [mm(k, kt) for k, kt in zip(ks, kts)]
    couplings, mixed = [], []
    for h in range(count):
        i = h // 2
        gap = cum[:, h : h + 1] - rows[h : h + 1]
        mix = jnp.where(same, jnp.exp(jnp.minimum(gap, 0.0)), 0.0) * rk_row[i]
        couplings.append(jnp.where(strict, (cols[:, 8 + h : 9 + h] * rk[i]) * (mix * kk[i]), 0.0))
        mixed.append(mix)
    if q_wait:
        q_wait()
    qs = [q_ref[:, pl.ds(pl.multiple_of((groups + i) * DK, DK), DK)] for i in range(count // 2)]
    rq = [unit(q) * DK ** (-0.5) for q in qs]
    qk = [mm(q, kt) for q, kt in zip(qs, kts)]
    for h in range(count):
        mixes[h] = rq[h // 2] * (mixed[h] * qk[h // 2])
    inv = inverses(couplings)
    if v_wait:
        v_wait()
    for h in range(count):
        i = h // 2
        entry_row = jnp.where(cont_row, jnp.exp(rows[h : h + 1]), 0.0)
        entry_col = jnp.where(cont_col, jnp.exp(cum[:, h : h + 1]), 0.0)
        beta_row = beta[h : h + 1]
        weighted = mm_left(inv[h] * (beta_row * entry_row * rk_row[i]), ks[i])
        pseudo = mm_left(inv[h] * beta_row, v_ref[:, pl.ds(pl.multiple_of((heads + h) * DV, DV), DV)])
        pair = jnp.concatenate([weighted, pseudo], 1)
        both[h] = pair
        reads[h] = (entry_col * rq[i]) * qs[i].astype(f32)
        last_gap = jnp.minimum(cum[N - 1 : N, h : h + 1] - cum[:, h : h + 1], 0.0)
        last_keys = jnp.where(last_col, jnp.exp(last_gap), 0.0) * rk[i]
        written = mm_right(kts[i], last_keys * pair)
        pack_wide(out, (h,), entry_row[:, N - 1 :], written[:, :DK], written[:, DK:], first_doc, last_doc)


def send_maps(q, k, v, g, b, seg, out, mixes, both, reads, q_in, k_in, v_in, g_in, b_in, seg_in, sems):
    moves = [
        pltpu.make_async_copy(src, dst, sems.at[i])
        for i, (src, dst) in enumerate(
            ((seg, seg_in), (g, g_in), (b, b_in), (k, k_in), (q, q_in), (v, v_in))
        )
    ]
    for move in moves:
        move.start()
    for move in moves[:4]:
        move.wait()
    heads = (1 - places()[0]) * out.shape[0]
    waits = (moves[4].wait, moves[5].wait)
    local_maps(heads, q_in, k_in, v_in, g_in, b_in, seg_in, out, mixes, both, reads, waits)


def own_maps(q, k, v, g, b, seg, out, mixes, both, reads):
    local_maps(places()[0] * out.shape[0], q, k, v, g, b, seg, out, mixes, both, reads)


def local_reads(mixes0, both0, reads0, mixes1, both1, reads1, gate, local, read, silu):
    core = places()[0]
    half = mixes0.shape[0]
    width = half * DV
    for part, (mixes, both, reads) in enumerate(((mixes0, both0, reads0), (mixes1, both1, reads1))):
        for h in range(half):
            mixed = mm_both(mixes[h], both[h])
            local[part * half + h] = mixed[:, DK:]
            read[part * half + h] = reads[h] - mixed[:, :DK]
        first = pl.multiple_of((core ^ part) * width, width)
        z = gate[:, pl.ds(first, width)].astype(f32)
        silu[:, part * width : (part + 1) * width] = z / (1.0 + jnp.exp(-z))


def pair_maps(own, got, *refs):
    outs, pair = refs[:4], refs[4]
    core, low, high, _ = places()
    pair[core] = own[...]
    pair[1 - core] = got[...]
    for s in range(4):
        j = low ^ s ^ (2 * high)
        pack(outs[s], *compose(parse_wide(pair[0, j]), parse_wide(pair[1, j])))


def quad_maps(m0, m1, m2, m3, total, prefix, prefix_row, maps):
    low = places()[1]
    for s, m in enumerate((m0, m1, m2, m3)):
        maps[low ^ s] = m[...]
    c, d, b, first, last = parse(maps[0])
    current = (c, d.astype(f32), b, first, last)
    for t in range(3):
        later = parse(maps[t + 1])
        prefix[t, :, :DK] = current[1]
        prefix[t, :, DK:] = current[2]
        row = iota((8, DK), 0)
        link = jnp.where(current[4] == later[3], 1.0, 0.0)
        prefix_row[t] = jnp.where(row == 0, current[0], link)
        current = compose(current, later)
    pack(total, *current)


def row_map(own, got, out, maps):
    high = places()[2]
    maps[high] = own[...]
    maps[1 - high] = got[...]
    pack(out, *compose(parse(maps[0]), parse(maps[1])))


def scan_states(r0, r1, r2, r3, own, got, prefix, prefix_row, o0, o1, o2, o3, maps, halves, final, pay):
    _, low, high, y = places()
    for s, r in enumerate((r0, r1, r2, r3)):
        maps[(y + 4 - s) % 4] = r[...]
    halves[high] = own[...]
    halves[1 - high] = got[...]
    state = jnp.zeros((DK, DV), f32)
    incoming = state
    before = jnp.full((1, DK), -1.0, f32)
    for t in range(4):
        row = parse(maps[t])
        entering = jnp.where(before == row[3], 1.0, 0.0) * state
        incoming = jnp.where(y == t, entering, incoming)
        state = apply_map(row, 1.0, entering)
        before = row[4]
    final[...] = state
    first_half = parse(halves[0])
    link = jnp.where(first_half[4] == parse(halves[1])[3], 1.0, 0.0)
    start = jnp.where(high == 1, apply_map(first_half, link, incoming), incoming)
    for t in range(4):
        here = start
        if t:
            c, link = prefix_row[t - 1, 0:1], prefix_row[t - 1, 1:2]
            here = apply_map((c, prefix[t - 1, :, :DK], prefix[t - 1, :, DK:]), link, start)
        pay[t, :DK] = here.astype(bf16)
        rows = final[pl.ds(4 * (y * 8 + high * 4 + t), 4)]
        hi = rows.astype(bf16).astype(f32)
        pay[t, DK:] = jnp.concatenate([hi, rows - hi, jnp.zeros((8, DV), f32)], 0).astype(bf16)
    for s, o in enumerate((o0, o1, o2, o3)):
        o[...] = pay[low ^ s]


def pair_states(s0, s1, s2, s3, own, got, own_out, send_out, pair, states, starts):
    core, low, high, _ = places()
    pair[core] = own[...]
    pair[1 - core] = got[...]
    for s, ref in enumerate((s0, s1, s2, s3)):
        starts[low ^ s ^ (2 * high)] = ref[...]
    for j in range(own.shape[0]):
        c, d, b, _, last = parse_wide(pair[0, j])
        link = jnp.where(last == parse_wide(pair[1, j])[3], 1.0, 0.0)
        start = starts[j, :DK]
        states[0, j, :DK] = start.astype(f32)
        states[1, j, :DK] = link * (c * start.astype(f32) - mm_left(d, start) + b)
        rows = starts[j, DK:].astype(f32)
        rows = jnp.concatenate([rows[:4] + rows[4:8], rows[8:12]], 0)
        states[0, j, DK:] = rows
        states[1, j, DK:] = rows
    own_out[...] = states[core]
    send_out[...] = states[1 - core]


def project(own, got, local, read, silu, w, acc, o1, o2, o3, tail, normed, total, lasts):
    core = places()[0]
    x = lax.axis_index("head")
    half = own.shape[0]
    width = half * DV
    for part, states in enumerate((own, got)):
        gated = []
        for h in range(half):
            at = part * half + h
            attention = local[at] + mm_both(read[at], states[h, :DK])
            mean_square = jnp.mean(attention * attention, axis=-1, keepdims=True)
            weight = lax.rsqrt(mean_square + EPS) * silu[:, at * DV : (at + 1) * DV]
            gated.append((attention * weight).astype(bf16))
            lasts[(core ^ part) * half + h] = states[h, DK:]
        first = pl.multiple_of((core ^ part) * width, width)
        normed[:, pl.ds(first, width)] = jnp.concatenate(gated, 1)
    finals = []
    for h in range(2 * half):
        rows = lasts[h]
        finals.append(jnp.where(core == 0, rows[0:2], rows[2:4]))
    finals = jnp.concatenate(finals, 0)
    hi = finals.astype(bf16).astype(f32)
    tail[...] = jnp.concatenate([hi, finals - hi], 0).astype(bf16)
    total[...] = mm(normed[...], w[...])
    acc[...] = total[pl.ds(x * 32, 32)]
    width = total.shape[1]
    for s, o in enumerate((o1, o2, o3)):
        o[:, :width] = total[pl.ds((x ^ (s + 1)) * 32, 32)].astype(bf16)
        o[:, width:] = tail[...]


def finish(order, acc, r1, r2, r3, tail, out, decode, final):
    x = lax.axis_index("head")
    total = acc[...]
    width = total.shape[1]
    for r in (r1, r2, r3):
        total = total + r[:, :width].astype(f32)
    out[...] = total.astype(bf16)
    slots = decode.shape[0]
    for s, block in enumerate((tail[...], r1[:, width:], r2[:, width:], r3[:, width:])):
        block = block.astype(f32)
        rows = block[:16] + block[16:]
        for h in range(slots):
            line = jnp.concatenate([rows[2 * h : 2 * h + 1], rows[2 * h + 1 : 2 * h + 2]], 1)
            final[pl.ds((x ^ s) * slots + h, 1)] = line
    for i in range(slots):
        decode[i : i + 1] = final[pl.ds(order[x * slots + i], 1)]


def shape(dims, dtype=bf16):
    return pltpu.VMEM(dims, dtype)


def call(kernel, outs, scratch, *args, smem=0, hbm=(), flops=None):
    specs = [pl.BlockSpec(memory_space=pltpu.SMEM)] * smem
    specs += [
        pl.BlockSpec(memory_space=pltpu.HBM if i in hbm else pltpu.VMEM) for i in range(smem, len(args))
    ]
    args = [
        a if i < smem else pltpu.with_memory_space_constraint(a, pltpu.HBM if i in hbm else pltpu.VMEM)
        for i, a in enumerate(args)
    ]
    cost = None if flops is None else pl.CostEstimate(flops=flops, transcendentals=0, bytes_accessed=0)
    return pl.pallas_call(
        kernel,
        out_shape=outs,
        scratch_shapes=scratch,
        in_specs=specs,
        cost_estimate=cost,
        compiler_params=pltpu.CompilerParams(vmem_limit_bytes=24 * 2**20),
    )(*args)


def xor_peers(count, bit):
    return [(i, i ^ bit) for i in range(count)]


def per_device(
    queries, keys, values, out_gate, log_decay, write_strength, segment_ids, head_order, out_weight
):
    heads = values.shape[1] // DV
    half = heads // 2
    peers = lax.axis_size("ctx")
    model = out_weight.shape[1]
    wide = (N + 8, 256)
    block = (ROWS, 256)
    block3 = (ROWS, 256)
    seg = segment_ids.reshape(1, N)
    maps = [
        shape((half,) + wide, f32),
        shape((half, N, N), f32),
        shape((half, N, 256), f32),
        shape((half, N, DK), f32),
    ]
    inputs = (queries, keys, values, log_decay.T, write_strength.T, seg)
    send, mixes1, both1, reads1, *held = call(
        send_maps,
        maps + [shape(a.shape, a.dtype) for a in inputs],
        [pltpu.SemaphoreType.DMA((6,))],
        *inputs,
        hbm=range(6),
    )
    got = lax.ppermute(send, "ctx", xor_peers(peers, 1))
    own, mixes0, both0, reads0 = call(own_maps, maps, [], *held, flops=10**9)
    m0, m1, m2, m3 = call(
        pair_maps,
        [shape(block)] * 4,
        [pltpu.VMEM((2, half) + wide, f32)],
        own, got,
    )
    m1, m2, m3 = [lax.ppermute(m, "ctx", xor_peers(peers, 2 * s)) for s, m in ((1, m1), (2, m2), (3, m3))]
    local, read, silu = call(
        local_reads,
        [shape((heads, N, DV), f32), shape((heads, N, DK), f32), shape((N, heads * DV), f32)],
        [],
        mixes0, both0, reads0, mixes1, both1, reads1, out_gate,
        flops=2 * 10**9,
    )
    total, prefix, prefix_row = call(
        quad_maps,
        [shape(block3), shape((3, DK, 256), f32), shape((3, 8, DK), f32)],
        [pltpu.VMEM((4,) + block, bf16)],
        m0, m1, m2, m3,
    )
    total_got = lax.ppermute(total, "ctx", xor_peers(peers, 12))
    r0 = call(
        row_map,
        shape(block3),
        [pltpu.VMEM((2,) + block3, bf16)],
        total, total_got,
    )
    rows = [[(i, (i + 16 * s) % peers) for i in range(peers)] for s in (1, 2, 3)]
    rows[2] = [(i, i - 16) for i in range(peers // 2, peers)]
    r1, r2, r3 = [lax.ppermute(r0, "ctx", pairs) for pairs in rows]
    s0, s1, s2, s3 = call(
        scan_states,
        [shape((ROWS, DV))] * 4,
        [
            pltpu.VMEM((4,) + block3, bf16),
            pltpu.VMEM((2,) + block3, bf16),
            pltpu.VMEM((DK, DV), f32),
            pltpu.VMEM((4, ROWS, DV), bf16),
        ],
        r0, r1, r2, r3, total, total_got, prefix, prefix_row,
    )
    s1, s2, s3 = [lax.ppermute(m, "ctx", xor_peers(peers, 2 * s)) for s, m in ((1, s1), (2, s2), (3, s3))]
    own_state, send_state = call(
        pair_states,
        [shape((half, N + 8, DV), f32)] * 2,
        [
            pltpu.VMEM((2, half) + wide, f32),
            pltpu.VMEM((2, half, N + 8, DV), f32),
            pltpu.VMEM((half, ROWS, DV), bf16),
        ],
        s0, s1, s2, s3, own, got,
    )
    got_state = lax.ppermute(send_state, "ctx", xor_peers(peers, 1))
    acc, o1, o2, o3, tail = call(
        project,
        [shape((32, model), f32)] + [shape((32, model + DV))] * 3 + [shape((32, DV))],
        [
            pltpu.VMEM((N, heads * DV), bf16),
            pltpu.VMEM((N, model), f32),
            pltpu.VMEM((heads, 8, DV), f32),
        ],
        own_state, got_state, local, read, silu, out_weight,
    )
    o1, o2, o3 = [lax.ppermute(o, "head", xor_peers(4, s)) for s, o in ((1, o1), (2, o2), (3, o3))]
    return call(
        finish,
        [jax.ShapeDtypeStruct((32, model), bf16), jax.ShapeDtypeStruct((heads, 256), f32)],
        [pltpu.VMEM((4 * heads, 256), f32)],
        head_order, acc, o1, o2, o3, tail,
        smem=1,
    )


def solution(mesh):
    in_specs = (
        P("ctx", "head"),
        P("ctx", "head"),
        P("ctx", "head"),
        P("ctx", "head"),
        P("ctx", "head"),
        P("ctx", "head"),
        P("ctx"),
        P(),
        P("head", None),
    )
    out_specs = (P(("ctx", "head"), None), P("head", "ctx"))

    def run(*args):
        return tuple(per_device(*args))

    return jax.shard_map(run, mesh=mesh, in_specs=in_specs, out_specs=out_specs, check_vma=False)
```

```python
import jax
import jax.numpy as jnp
from jax import lax
from jax.experimental import pallas as pl
from jax.experimental.pallas import tpu as pltpu
from jax.sharding import PartitionSpec as P


f32 = jnp.float32
bf16 = jnp.bfloat16
DK = 128
DV = 128
N = 128
ROWS = N + 16
EPS = 1e-06


def mm(a, b):
    return jnp.dot(a, b, preferred_element_type=f32)


def split(x):
    hi = x.astype(bf16)
    return hi, (x - hi.astype(f32)).astype(bf16)


def mm_left(a, b):
    hi, lo = split(a)
    return mm(jnp.concatenate([hi, lo], 1), jnp.concatenate([b, b], 0))


def mm_right(a, b):
    hi, lo = split(b)
    return mm(jnp.concatenate([a, a], 1), jnp.concatenate([hi, lo], 0))


def mm_both(a, b):
    ah, al = split(a)
    bh, bl = split(b)
    return mm(jnp.concatenate([ah, al], 1), jnp.concatenate([bh, bh], 0)) + mm(ah, bl)


def iota(shape, axis):
    return lax.broadcasted_iota(jnp.int32, shape, axis)


def places():
    ctx = lax.axis_index("ctx")
    return ctx % 2, (ctx // 2) % 4, (ctx // 8) % 2, ctx // 16


def lines(shape, values):
    row = iota(shape, 0)
    out = jnp.zeros(shape, f32)
    for i, value in enumerate(values):
        out = jnp.where(row == i, jnp.broadcast_to(value[:, :1], shape), out)
    return out


def pack_wide(ref, at, c, d, b, first, last):
    ref[at + (pl.ds(0, N), pl.ds(0, DK))] = d
    ref[at + (pl.ds(0, N), pl.ds(DK, DV))] = b
    ref[at + (pl.ds(N, 8), slice(None))] = lines((8, 256), (c, first, last))


def parse_wide(block):
    tail = block[N:, :DK]
    return tail[0:1], block[:N, :DK], block[:N, DK:], tail[1:2], tail[2:3]


def pack(ref, c, d, b, first, last):
    c0 = c.astype(bf16).astype(f32)
    c1 = (c - c0).astype(bf16).astype(f32)
    ref[:N, :DK] = d.astype(bf16)
    hi = b.astype(bf16)
    ref[:N, DK : 2 * DK] = hi
    if ref.shape[1] > 2 * DK:
        ref[:N, 2 * DK :] = (b - hi.astype(f32)).astype(bf16)
    ref[N:] = lines((16, ref.shape[1]), (c0, c1, c - c0 - c1, first, last)).astype(bf16)


def parse(block):
    tail = block[N:, :DK].astype(f32)
    c = tail[0:1] + tail[1:2] + tail[2:3]
    b = block[:N, DK : 2 * DK].astype(f32)
    if block.shape[1] > 2 * DK:
        b = b + block[:N, 2 * DK :].astype(f32)
    return c, block[:N, :DK], b, tail[3:4], tail[4:5]


def times(d, x):
    return mm_right(d, x) if d.dtype == bf16 else mm_both(d, x)


def compose(earlier, later):
    ce, de, be, fe, le = earlier
    cl, dl, bl, fl, ll = later
    link = jnp.where(le == fl, 1.0, 0.0)
    de = de.astype(f32)
    moved = times(dl, jnp.concatenate([de, be], 1))
    cl = cl * link
    d = cl * de + (link * ce) * dl.astype(f32) - link * moved[:, :DK]
    b = cl * be - link * moved[:, DK:] + bl
    return cl * ce, d, b, fe, ll


def apply_map(parts, link, state):
    c, d, b = parts[:3]
    return link * (c * state - times(d, state) + b)


def inverses(couplings):
    ii, jj = iota((N, N), 0), iota((N, N), 1)
    eye = jnp.where(ii == jj, 1.0, 0.0)
    inside = (ii // 16) == (jj // 16)
    squared = [jnp.where(inside, c, 0.0) for c in couplings]
    inv = [eye - s for s in squared]
    for _ in range(3):
        squared = [mm_both(s, s) for s in squared]
        inv = [x + mm_both(x, s) for x, s in zip(inv, squared)]
    for size in (16, 32, 64):
        odd = range(size, N, 2 * size)
        sibling = (ii // (2 * size)) == (jj // (2 * size))
        ring = sibling & ((ii // size) != (jj // size))

        def take(x):
            return jnp.concatenate([x[r : r + size] for r in odd], 0)

        def spread(x):
            gap = jnp.zeros((size, N), f32)
            return jnp.concatenate([y for i in range(len(odd)) for y in (gap, x[i * size : (i + 1) * size])], 0)

        below = [mm_both(take(jnp.where(ring, c, 0.0)), x) for c, x in zip(couplings, inv)]
        inv = [x - spread(mm_both(take(x), spread(y))) for x, y in zip(inv, below)]
    return inv


def unit(x):
    x = x.astype(f32)
    return lax.rsqrt(jnp.sum(x * x, axis=-1, keepdims=True) + EPS)


def local_maps(heads, k_ref, v_ref, g_ref, b_ref, seg_ref, out, mixes, both, sums, v_wait=None):
    groups = heads // 2
    ii, jj = iota((N, N), 0), iota((N, N), 1)
    doc_row = jnp.broadcast_to(seg_ref[...].astype(f32), (N, N))
    doc_col = doc_row.T
    same = (doc_row == doc_col) & (ii >= jj)
    strict = same & (ii > jj)
    cont_row = doc_row[0:1] == doc_col[0:1]
    last_col = doc_col[:, 0:1] == doc_row[:, N - 1 : N]
    first_doc, last_doc = doc_col[0:1], doc_col[N - 1 : N]
    upper = jnp.where(ii <= jj, 1.0, 0.0).astype(bf16)
    count = out.shape[0]
    g = g_ref[pl.ds(heads, count)]
    beta = b_ref[pl.ds(heads, count)]
    g = jnp.concatenate([g, jnp.zeros((8 - count, N), f32)], 0)
    g0 = g.astype(bf16)
    g1 = (g - g0.astype(f32)).astype(bf16)
    g2 = (g - g0.astype(f32) - g1.astype(f32)).astype(bf16)
    rows = mm(g0, upper) + mm(g1, upper) + mm(g2, upper)
    ks = [k_ref[:, pl.ds(pl.multiple_of((groups + i) * DK, DK), DK)] for i in range(count // 2)]
    cols = jnp.concatenate([rows, beta, jnp.zeros((N - 8 - count, N), f32)], 0).T
    cum = cols[:, :count]
    rk = [unit(k) for k in ks]
    rk_row = [jnp.broadcast_to(r, (N, N)).T[0:1] for r in rk]
    kts = [k.astype(f32).T.astype(bf16) for k in ks]
    kk = [mm(k, kt) for k, kt in zip(ks, kts)]
    couplings = []
    sums[...] = cols
    for h in range(count):
        i = h // 2
        gap = cum[:, h : h + 1] - rows[h : h + 1]
        mix = jnp.where(same, jnp.exp(jnp.minimum(gap, 0.0)), 0.0) * rk_row[i]
        couplings.append(jnp.where(strict, (cols[:, 8 + h : 9 + h] * rk[i]) * (mix * kk[i]), 0.0))
        mixes[h] = mix
    inv = inverses(couplings)
    if v_wait:
        v_wait()
    for h in range(count):
        i = h // 2
        entry_row = jnp.where(cont_row, jnp.exp(rows[h : h + 1]), 0.0)
        beta_row = beta[h : h + 1]
        weighted = mm_left(inv[h] * (beta_row * entry_row * rk_row[i]), ks[i])
        pseudo = mm_left(inv[h] * beta_row, v_ref[:, pl.ds(pl.multiple_of((heads + h) * DV, DV), DV)])
        pair = jnp.concatenate([weighted, pseudo], 1)
        both[h] = pair
        last_gap = jnp.minimum(cum[N - 1 : N, h : h + 1] - cum[:, h : h + 1], 0.0)
        last_keys = jnp.where(last_col, jnp.exp(last_gap), 0.0) * rk[i]
        written = mm_right(kts[i], last_keys * pair)
        pack_wide(out, (h,), entry_row[:, N - 1 :], written[:, :DK], written[:, DK:], first_doc, last_doc)


def send_maps(k, v, g, b, seg, out, mixes, both, sums, k_in, v_in, g_in, b_in, seg_in, sems):
    moves = [
        pltpu.make_async_copy(src, dst, sems.at[i])
        for i, (src, dst) in enumerate(((k, k_in), (seg, seg_in), (g, g_in), (b, b_in), (v, v_in)))
    ]
    for move in moves:
        move.start()
    for move in moves[:4]:
        move.wait()
    heads = (1 - places()[0]) * out.shape[0]
    local_maps(heads, k_in, v_in, g_in, b_in, seg_in, out, mixes, both, sums, moves[4].wait)


def own_maps(k, v, g, b, seg, out, mixes, both, sums):
    local_maps(places()[0] * out.shape[0], k, v, g, b, seg, out, mixes, both, sums)


def local_reads(mixes0, both0, sums0, mixes1, both1, sums1, q_ref, k_ref, seg_ref, gate, local, read, silu):
    core = places()[0]
    half = mixes0.shape[0]
    width = half * DV
    docs = jnp.broadcast_to(seg_ref[...].astype(f32), (N, N))
    cont_col = docs.T[:, 0:1] == docs[:, 0:1]
    for part, (mixes, both, sums) in enumerate(((mixes0, both0, sums0), (mixes1, both1, sums1))):
        first = (core ^ part) * half
        for h in range(half):
            if h % 2 == 0:
                lanes = pl.ds(pl.multiple_of((first // 2 + h // 2) * DK, DK), DK)
                q = q_ref[:, lanes]
                rq = unit(q) * DK ** (-0.5)
                qk = rq * lax.dot_general(q, k_ref[:, lanes], (((1,), (1,)), ((), ())), preferred_element_type=f32)
            at = part * half + h
            mixed = mm_both(mixes[h] * qk, both[h])
            entry_col = jnp.where(cont_col, jnp.exp(sums[:, h : h + 1]), 0.0)
            local[at] = mixed[:, DK:]
            read[at] = (entry_col * rq) * q.astype(f32) - mixed[:, :DK]
        first = pl.multiple_of(first * DV, width)
        z = gate[:, pl.ds(first, width)].astype(f32)
        silu[:, part * width : (part + 1) * width] = z / (1.0 + jnp.exp(-z))


def pair_maps(own, got, *refs):
    outs, pair = refs[:4], refs[4]
    core, low, high, _ = places()
    pair[core] = own[...]
    pair[1 - core] = got[...]
    for s in range(4):
        j = low ^ s ^ (2 * high)
        pack(outs[s], *compose(parse_wide(pair[0, j]), parse_wide(pair[1, j])))


def quad_maps(m0, m1, m2, m3, total, prefix, prefix_row, maps):
    low = places()[1]
    for s, m in enumerate((m0, m1, m2, m3)):
        maps[low ^ s] = m[...]
    c, d, b, first, last = parse(maps[0])
    current = (c, d.astype(f32), b, first, last)
    for t in range(3):
        later = parse(maps[t + 1])
        prefix[t, :, :DK] = current[1]
        prefix[t, :, DK:] = current[2]
        row = iota((8, DK), 0)
        link = jnp.where(current[4] == later[3], 1.0, 0.0)
        prefix_row[t] = jnp.where(row == 0, current[0], link)
        current = compose(current, later)
    pack(total, *current)


def row_map(own, got, out, maps):
    high = places()[2]
    maps[high] = own[...]
    maps[1 - high] = got[...]
    pack(out, *compose(parse(maps[0]), parse(maps[1])))


def scan_states(r0, r1, r2, r3, own, got, prefix, prefix_row, o0, o1, o2, o3, maps, halves, final, pay):
    _, low, high, y = places()
    for s, r in enumerate((r0, r1, r2, r3)):
        maps[(y + 4 - s) % 4] = r[...]
    halves[high] = own[...]
    halves[1 - high] = got[...]

    def after(newer, older, there):
        link = jnp.where(older[4] == newer[3], there, 0.0)
        return apply_map(newer, 1.0, link * older[2])

    row = parse(maps[y])
    last, older = parse(maps[(y + 3) % 4]), parse(maps[(y + 2) % 4])
    reached = after(last, older, jnp.where(y >= 2, 1.0, 0.0))
    incoming = jnp.where(last[4] == row[3], jnp.where(y >= 1, 1.0, 0.0), 0.0) * reached
    final[...] = after(parse(maps[3]), parse(maps[2]), 1.0)
    first_half = parse(halves[0])
    link = jnp.where(first_half[4] == parse(halves[1])[3], 1.0, 0.0)
    start = jnp.where(high == 1, apply_map(first_half, link, incoming), incoming)
    for t in range(4):
        here = start
        if t:
            c, link = prefix_row[t - 1, 0:1], prefix_row[t - 1, 1:2]
            here = apply_map((c, prefix[t - 1, :, :DK], prefix[t - 1, :, DK:]), link, start)
        pay[t, :DK] = here.astype(bf16)
        rows = final[pl.ds(4 * (y * 8 + high * 4 + t), 4)]
        hi = rows.astype(bf16).astype(f32)
        pay[t, DK:] = jnp.concatenate([hi, rows - hi, jnp.zeros((8, DV), f32)], 0).astype(bf16)
    for s, o in enumerate((o0, o1, o2, o3)):
        o[...] = pay[low ^ s]


def pair_states(s0, s1, s2, s3, own, got, own_out, send_out, pair, states, starts):
    core, low, high, _ = places()
    pair[core] = own[...]
    pair[1 - core] = got[...]
    for s, ref in enumerate((s0, s1, s2, s3)):
        starts[low ^ s ^ (2 * high)] = ref[...]
    for j in range(own.shape[0]):
        c, d, b, _, last = parse_wide(pair[0, j])
        link = jnp.where(last == parse_wide(pair[1, j])[3], 1.0, 0.0)
        start = starts[j, :DK]
        states[0, j, :DK] = start.astype(f32)
        states[1, j, :DK] = link * (c * start.astype(f32) - mm_left(d, start) + b)
        rows = starts[j, DK:].astype(f32)
        rows = jnp.concatenate([rows[:4] + rows[4:8], rows[8:12]], 0)
        states[0, j, DK:] = rows
        states[1, j, DK:] = rows
    own_out[...] = states[core]
    send_out[...] = states[1 - core]


def project(own, got, local, read, silu, w, acc, o1, o2, o3, tail, normed, total, lasts):
    core = places()[0]
    x = lax.axis_index("head")
    half = own.shape[0]
    width = half * DV
    for part, states in enumerate((own, got)):
        gated = []
        for h in range(half):
            at = part * half + h
            attention = local[at] + mm_both(read[at], states[h, :DK])
            mean_square = jnp.mean(attention * attention, axis=-1, keepdims=True)
            weight = lax.rsqrt(mean_square + EPS) * silu[:, at * DV : (at + 1) * DV]
            gated.append((attention * weight).astype(bf16))
            lasts[(core ^ part) * half + h] = states[h, DK:]
        first = pl.multiple_of((core ^ part) * width, width)
        normed[:, pl.ds(first, width)] = jnp.concatenate(gated, 1)
    finals = []
    for h in range(2 * half):
        rows = lasts[h]
        finals.append(jnp.where(core == 0, rows[0:2], rows[2:4]))
    finals = jnp.concatenate(finals, 0)
    hi = finals.astype(bf16).astype(f32)
    tail[...] = jnp.concatenate([hi, finals - hi], 0).astype(bf16)
    total[...] = mm(normed[...], w[...])
    acc[...] = total[pl.ds(x * 32, 32)]
    width = total.shape[1]
    for s, o in enumerate((o1, o2, o3)):
        o[:, :width] = total[pl.ds((x ^ (s + 1)) * 32, 32)].astype(bf16)
        o[:, width:] = tail[...]


def finish(order, acc, r1, r2, r3, tail, out, decode, final):
    x = lax.axis_index("head")
    total = acc[...]
    width = total.shape[1]
    for r in (r1, r2, r3):
        total = total + r[:, :width].astype(f32)
    out[...] = total.astype(bf16)
    slots = decode.shape[0]
    for s, block in enumerate((tail[...], r1[:, width:], r2[:, width:], r3[:, width:])):
        block = block.astype(f32)
        rows = block[:16] + block[16:]
        for h in range(slots):
            line = jnp.concatenate([rows[2 * h : 2 * h + 1], rows[2 * h + 1 : 2 * h + 2]], 1)
            final[pl.ds((x ^ s) * slots + h, 1)] = line
    for i in range(slots):
        decode[i : i + 1] = final[pl.ds(order[x * slots + i], 1)]


def shape(dims, dtype=bf16):
    return pltpu.VMEM(dims, dtype)


def call(kernel, outs, scratch, *args, smem=0, hbm=(), flops=None):
    specs = [pl.BlockSpec(memory_space=pltpu.SMEM)] * smem
    specs += [
        pl.BlockSpec(memory_space=pltpu.HBM if i in hbm else pltpu.VMEM) for i in range(smem, len(args))
    ]
    args = [
        a if i < smem else pltpu.with_memory_space_constraint(a, pltpu.HBM if i in hbm else pltpu.VMEM)
        for i, a in enumerate(args)
    ]
    cost = None if flops is None else pl.CostEstimate(flops=flops, transcendentals=0, bytes_accessed=0)
    return pl.pallas_call(
        kernel,
        out_shape=outs,
        scratch_shapes=scratch,
        in_specs=specs,
        cost_estimate=cost,
        compiler_params=pltpu.CompilerParams(vmem_limit_bytes=24 * 2**20),
    )(*args)


def xor_peers(count, bit):
    return [(i, i ^ bit) for i in range(count)]


def per_device(
    queries, keys, values, out_gate, log_decay, write_strength, segment_ids, head_order, out_weight
):
    heads = values.shape[1] // DV
    half = heads // 2
    peers = lax.axis_size("ctx")
    model = out_weight.shape[1]
    wide = (N + 8, 256)
    block = (ROWS, 256)
    block3 = (ROWS, 256)
    seg = segment_ids.reshape(1, N)
    maps = [
        shape((half,) + wide, f32),
        shape((half, N, N), f32),
        shape((half, N, 256), f32),
        shape((N, N), f32),
    ]
    inputs = (keys, values, log_decay.T, write_strength.T, seg)
    send, mixes1, both1, sums1, *held = call(
        send_maps,
        maps + [shape(a.shape, a.dtype) for a in inputs],
        [pltpu.SemaphoreType.DMA((5,))],
        *inputs,
        hbm=range(5),
    )
    got = lax.ppermute(send, "ctx", xor_peers(peers, 1))
    own, mixes0, both0, sums0 = call(own_maps, maps, [], *held, flops=10**9)
    m0, m1, m2, m3 = call(
        pair_maps,
        [shape(block)] * 4,
        [pltpu.VMEM((2, half) + wide, f32)],
        own, got,
    )
    m1, m2, m3 = [lax.ppermute(m, "ctx", xor_peers(peers, 2 * s)) for s, m in ((1, m1), (2, m2), (3, m3))]
    local, read, silu = call(
        local_reads,
        [shape((heads, N, DV), f32), shape((heads, N, DK), f32), shape((N, heads * DV), f32)],
        [],
        mixes0, both0, sums0, mixes1, both1, sums1, queries, held[0], held[4], out_gate,
        flops=2 * 10**9,
    )
    total, prefix, prefix_row = call(
        quad_maps,
        [shape(block3), shape((3, DK, 256), f32), shape((3, 8, DK), f32)],
        [pltpu.VMEM((4,) + block, bf16)],
        m0, m1, m2, m3,
    )
    total_got = lax.ppermute(total, "ctx", xor_peers(peers, 12))
    r0 = call(
        row_map,
        shape(block3),
        [pltpu.VMEM((2,) + block3, bf16)],
        total, total_got,
    )
    rows = [[(i, (i + 16 * s) % peers) for i in range(peers)] for s in (1, 2, 3)]
    rows[2] = [(i, i - 16) for i in range(peers // 2, peers)]
    r1, r2, r3 = [lax.ppermute(r0, "ctx", pairs) for pairs in rows]
    s0, s1, s2, s3 = call(
        scan_states,
        [shape((ROWS, DV))] * 4,
        [
            pltpu.VMEM((4,) + block3, bf16),
            pltpu.VMEM((2,) + block3, bf16),
            pltpu.VMEM((DK, DV), f32),
            pltpu.VMEM((4, ROWS, DV), bf16),
        ],
        r0, r1, r2, r3, total, total_got, prefix, prefix_row,
    )
    s1, s2, s3 = [lax.ppermute(m, "ctx", xor_peers(peers, 2 * s)) for s, m in ((1, s1), (2, s2), (3, s3))]
    own_state, send_state = call(
        pair_states,
        [shape((half, N + 8, DV), f32)] * 2,
        [
            pltpu.VMEM((2, half) + wide, f32),
            pltpu.VMEM((2, half, N + 8, DV), f32),
            pltpu.VMEM((half, ROWS, DV), bf16),
        ],
        s0, s1, s2, s3, own, got,
    )
    got_state = lax.ppermute(send_state, "ctx", xor_peers(peers, 1))
    acc, o1, o2, o3, tail = call(
        project,
        [shape((32, model), f32)] + [shape((32, model + DV))] * 3 + [shape((32, DV))],
        [
            pltpu.VMEM((N, heads * DV), bf16),
            pltpu.VMEM((N, model), f32),
            pltpu.VMEM((heads, 8, DV), f32),
        ],
        own_state, got_state, local, read, silu, out_weight,
    )
    o1, o2, o3 = [lax.ppermute(o, "head", xor_peers(4, s)) for s, o in ((1, o1), (2, o2), (3, o3))]
    return call(
        finish,
        [jax.ShapeDtypeStruct((32, model), bf16), jax.ShapeDtypeStruct((heads, 256), f32)],
        [pltpu.VMEM((4 * heads, 256), f32)],
        head_order, acc, o1, o2, o3, tail,
        smem=1,
    )


def solution(mesh):
    in_specs = (
        P("ctx", "head"),
        P("ctx", "head"),
        P("ctx", "head"),
        P("ctx", "head"),
        P("ctx", "head"),
        P("ctx", "head"),
        P("ctx"),
        P(),
        P("head", None),
    )
    out_specs = (P(("ctx", "head"), None), P("head", "ctx"))

    def run(*args):
        return tuple(per_device(*args))

    return jax.shard_map(run, mesh=mesh, in_specs=in_specs, out_specs=out_specs, check_vma=False)
```

```python
import jax
import jax.numpy as jnp
from jax import lax
from jax.experimental import pallas as pl
from jax.experimental.pallas import tpu as pltpu
from jax.sharding import PartitionSpec as P


f32 = jnp.float32
bf16 = jnp.bfloat16
DK = 128
DV = 128
N = 128
ROWS = N + 16
EPS = 1e-06


def mm(a, b):
    return jnp.dot(a, b, preferred_element_type=f32)


def split(x):
    hi = x.astype(bf16)
    return hi, (x - hi.astype(f32)).astype(bf16)


def mm_left(a, b):
    hi, lo = split(a)
    return mm(jnp.concatenate([hi, lo], 1), jnp.concatenate([b, b], 0))


def mm_right(a, b):
    hi, lo = split(b)
    return mm(jnp.concatenate([a, a], 1), jnp.concatenate([hi, lo], 0))


def mm_both(a, b):
    ah, al = split(a)
    bh, bl = split(b)
    return mm(jnp.concatenate([ah, al], 1), jnp.concatenate([bh, bh], 0)) + mm(ah, bl)


def iota(shape, axis):
    return lax.broadcasted_iota(jnp.int32, shape, axis)


def places():
    ctx = lax.axis_index("ctx")
    return ctx % 2, (ctx // 2) % 4, (ctx // 8) % 2, ctx // 16


def lines(shape, values):
    row = iota(shape, 0)
    out = jnp.zeros(shape, f32)
    for i, value in enumerate(values):
        out = jnp.where(row == i, jnp.broadcast_to(value[:, :1], shape), out)
    return out


def pack_wide(ref, at, c, d, b, first, last):
    ref[at + (pl.ds(0, N), pl.ds(0, DK))] = d
    ref[at + (pl.ds(0, N), pl.ds(DK, DV))] = b
    ref[at + (pl.ds(N, 8), slice(None))] = lines((8, 256), (c, first, last))


def parse_wide(block):
    tail = block[N:, :DK]
    return tail[0:1], block[:N, :DK], block[:N, DK:], tail[1:2], tail[2:3]


def pack(ref, c, d, b, first, last):
    c0 = c.astype(bf16).astype(f32)
    c1 = (c - c0).astype(bf16).astype(f32)
    ref[:N, :DK] = d.astype(bf16)
    hi = b.astype(bf16)
    ref[:N, DK : 2 * DK] = hi
    if ref.shape[1] > 2 * DK:
        ref[:N, 2 * DK :] = (b - hi.astype(f32)).astype(bf16)
    ref[N:] = lines((16, ref.shape[1]), (c0, c1, c - c0 - c1, first, last)).astype(bf16)


def parse(block):
    tail = block[N:, :DK].astype(f32)
    c = tail[0:1] + tail[1:2] + tail[2:3]
    b = block[:N, DK : 2 * DK].astype(f32)
    if block.shape[1] > 2 * DK:
        b = b + block[:N, 2 * DK :].astype(f32)
    return c, block[:N, :DK], b, tail[3:4], tail[4:5]


def times(d, x):
    return mm_right(d, x) if d.dtype == bf16 else mm_both(d, x)


def compose(earlier, later):
    ce, de, be, fe, le = earlier
    cl, dl, bl, fl, ll = later
    link = jnp.where(le == fl, 1.0, 0.0)
    de = de.astype(f32)
    moved = times(dl, jnp.concatenate([de, be], 1))
    cl = cl * link
    d = cl * de + (link * ce) * dl.astype(f32) - link * moved[:, :DK]
    b = cl * be - link * moved[:, DK:] + bl
    return cl * ce, d, b, fe, ll


def apply_map(parts, link, state):
    c, d, b = parts[:3]
    return link * (c * state - times(d, state) + b)


def inverses(couplings):
    ii, jj = iota((N, N), 0), iota((N, N), 1)
    eye = jnp.where(ii == jj, 1.0, 0.0)
    inside = (ii // 16) == (jj // 16)
    squared = [jnp.where(inside, c, 0.0) for c in couplings]
    inv = [eye - s for s in squared]
    for _ in range(3):
        squared = [mm_both(s, s) for s in squared]
        inv = [x + mm_both(x, s) for x, s in zip(inv, squared)]
    for size in (16, 32, 64):
        odd = range(size, N, 2 * size)
        sibling = (ii // (2 * size)) == (jj // (2 * size))
        ring = sibling & ((ii // size) != (jj // size))

        def take(x):
            return jnp.concatenate([x[r : r + size] for r in odd], 0)

        def spread(x):
            gap = jnp.zeros((size, N), f32)
            return jnp.concatenate([y for i in range(len(odd)) for y in (gap, x[i * size : (i + 1) * size])], 0)

        below = [mm_both(take(jnp.where(ring, c, 0.0)), x) for c, x in zip(couplings, inv)]
        inv = [x - spread(mm_both(take(x), spread(y))) for x, y in zip(inv, below)]
    return inv


def unit(x):
    x = x.astype(f32)
    return lax.rsqrt(jnp.sum(x * x, axis=-1, keepdims=True) + EPS)


def local_maps(heads, k_ref, v_ref, g_ref, b_ref, seg_ref, out, mixes, both, sums, v_wait=None):
    groups = heads // 2
    ii, jj = iota((N, N), 0), iota((N, N), 1)
    doc_row = jnp.broadcast_to(seg_ref[...].astype(f32), (N, N))
    doc_col = doc_row.T
    same = (doc_row == doc_col) & (ii >= jj)
    strict = same & (ii > jj)
    cont_row = doc_row[0:1] == doc_col[0:1]
    last_col = doc_col[:, 0:1] == doc_row[:, N - 1 : N]
    first_doc, last_doc = doc_col[0:1], doc_col[N - 1 : N]
    upper = jnp.where(ii <= jj, 1.0, 0.0).astype(bf16)
    count = out.shape[0]
    g = g_ref[pl.ds(heads, count)]
    beta = b_ref[pl.ds(heads, count)]
    g = jnp.concatenate([g, jnp.zeros((8 - count, N), f32)], 0)
    g0 = g.astype(bf16)
    g1 = (g - g0.astype(f32)).astype(bf16)
    g2 = (g - g0.astype(f32) - g1.astype(f32)).astype(bf16)
    rows = mm(g0, upper) + mm(g1, upper) + mm(g2, upper)
    ks = [k_ref[:, pl.ds(pl.multiple_of((groups + i) * DK, DK), DK)] for i in range(count // 2)]
    cols = jnp.concatenate([rows, beta, jnp.zeros((N - 8 - count, N), f32)], 0).T
    cum = cols[:, :count]
    rk = [unit(k) for k in ks]
    rk_row = [jnp.broadcast_to(r, (N, N)).T[0:1] for r in rk]
    kts = [k.astype(f32).T.astype(bf16) for k in ks]
    kk = [mm(k, kt) for k, kt in zip(ks, kts)]
    couplings = []
    sums[...] = cols
    for h in range(count):
        i = h // 2
        gap = cum[:, h : h + 1] - rows[h : h + 1]
        mix = jnp.where(same, jnp.exp(jnp.minimum(gap, 0.0)), 0.0) * rk_row[i]
        couplings.append(jnp.where(strict, (cols[:, 8 + h : 9 + h] * rk[i]) * (mix * kk[i]), 0.0))
        mixes[h] = mix
    inv = inverses(couplings)
    if v_wait:
        v_wait()
    for h in range(count):
        i = h // 2
        entry_row = jnp.where(cont_row, jnp.exp(rows[h : h + 1]), 0.0)
        beta_row = beta[h : h + 1]
        weighted = mm_left(inv[h] * (beta_row * entry_row * rk_row[i]), ks[i])
        pseudo = mm_left(inv[h] * beta_row, v_ref[:, pl.ds(pl.multiple_of((heads + h) * DV, DV), DV)])
        pair = jnp.concatenate([weighted, pseudo], 1)
        both[h] = pair
        last_gap = jnp.minimum(cum[N - 1 : N, h : h + 1] - cum[:, h : h + 1], 0.0)
        last_keys = jnp.where(last_col, jnp.exp(last_gap), 0.0) * rk[i]
        written = mm_right(kts[i], last_keys * pair)
        pack_wide(out, (h,), entry_row[:, N - 1 :], written[:, :DK], written[:, DK:], first_doc, last_doc)


def send_maps(k, v, g, b, seg, out, mixes, both, sums, k_in, v_in, g_in, b_in, seg_in, sems):
    moves = [
        pltpu.make_async_copy(src, dst, sems.at[i])
        for i, (src, dst) in enumerate(((k, k_in), (seg, seg_in), (g, g_in), (b, b_in), (v, v_in)))
    ]
    for move in moves:
        move.start()
    for move in moves[:4]:
        move.wait()
    heads = (1 - places()[0]) * out.shape[0]
    local_maps(heads, k_in, v_in, g_in, b_in, seg_in, out, mixes, both, sums, moves[4].wait)


def own_maps(k, v, g, b, seg, out, mixes, both, sums):
    local_maps(places()[0] * out.shape[0], k, v, g, b, seg, out, mixes, both, sums)


def local_reads(mixes0, both0, sums0, mixes1, both1, sums1, q_ref, k_ref, seg_ref, gate, local, read, silu):
    core = places()[0]
    half = mixes0.shape[0]
    width = half * DV
    docs = jnp.broadcast_to(seg_ref[...].astype(f32), (N, N))
    cont_col = docs.T[:, 0:1] == docs[:, 0:1]
    for part, (mixes, both, sums) in enumerate(((mixes0, both0, sums0), (mixes1, both1, sums1))):
        first = (core ^ part) * half
        for h in range(half):
            if h % 2 == 0:
                lanes = pl.ds(pl.multiple_of((first // 2 + h // 2) * DK, DK), DK)
                q = q_ref[:, lanes]
                rq = unit(q) * DK ** (-0.5)
                qk = rq * lax.dot_general(q, k_ref[:, lanes], (((1,), (1,)), ((), ())), preferred_element_type=f32)
            at = part * half + h
            mixed = mm_both(mixes[h] * qk, both[h])
            entry_col = jnp.where(cont_col, jnp.exp(sums[:, h : h + 1]), 0.0)
            local[at] = mixed[:, DK:]
            read[at] = (entry_col * rq) * q.astype(f32) - mixed[:, :DK]
        first = pl.multiple_of(first * DV, width)
        z = gate[:, pl.ds(first, width)].astype(f32)
        silu[:, part * width : (part + 1) * width] = z / (1.0 + jnp.exp(-z))


def pair_maps(own, got, *refs):
    outs, pair = refs[:4], refs[4]
    core, low, high, _ = places()
    pair[core] = own[...]
    pair[1 - core] = got[...]
    for s in range(4):
        j = low ^ s ^ (2 * high)
        pack(outs[s], *compose(parse_wide(pair[0, j]), parse_wide(pair[1, j])))


def quad_maps(m0, m1, m2, m3, total, prefix, prefix_row, maps):
    low = places()[1]
    for s, m in enumerate((m0, m1, m2, m3)):
        maps[low ^ s] = m[...]
    parts = [parse(maps[t]) for t in range(4)]
    wide = [(c, d.astype(f32), b, first, last) for c, d, b, first, last in parts]
    two = compose(wide[0], parts[1])
    pack(total, *compose(two, compose(wide[2], parts[3])))
    row = iota((8, DK), 0)
    for t, reached in enumerate((wide[0], two, compose(two, parts[2]))):
        prefix[t, :, :DK] = reached[1]
        prefix[t, :, DK:] = reached[2]
        link = jnp.where(reached[4] == parts[t + 1][3], 1.0, 0.0)
        prefix_row[t] = jnp.where(row == 0, reached[0], link)


def row_map(own, got, out, maps):
    high = places()[2]
    maps[high] = own[...]
    maps[1 - high] = got[...]
    pack(out, *compose(parse(maps[0]), parse(maps[1])))


def scan_states(r0, r1, r2, r3, own, got, prefix, prefix_row, o0, o1, o2, o3, maps, halves, final, pay):
    _, low, high, y = places()
    for s, r in enumerate((r0, r1, r2, r3)):
        maps[(y + 4 - s) % 4] = r[...]
    halves[high] = own[...]
    halves[1 - high] = got[...]

    def after(newer, older, there):
        link = jnp.where(older[4] == newer[3], there, 0.0)
        return apply_map(newer, 1.0, link * older[2])

    row = parse(maps[y])
    last, older = parse(maps[(y + 3) % 4]), parse(maps[(y + 2) % 4])
    reached = after(last, older, jnp.where(y >= 2, 1.0, 0.0))
    incoming = jnp.where(last[4] == row[3], jnp.where(y >= 1, 1.0, 0.0), 0.0) * reached
    final[...] = after(parse(maps[3]), parse(maps[2]), 1.0)
    first_half = parse(halves[0])
    link = jnp.where(first_half[4] == parse(halves[1])[3], 1.0, 0.0)
    start = jnp.where(high == 1, apply_map(first_half, link, incoming), incoming)
    for t in range(4):
        here = start
        if t:
            c, link = prefix_row[t - 1, 0:1], prefix_row[t - 1, 1:2]
            here = apply_map((c, prefix[t - 1, :, :DK], prefix[t - 1, :, DK:]), link, start)
        pay[t, :DK] = here.astype(bf16)
        rows = final[pl.ds(4 * (y * 8 + high * 4 + t), 4)]
        hi = rows.astype(bf16).astype(f32)
        pay[t, DK:] = jnp.concatenate([hi, rows - hi, jnp.zeros((8, DV), f32)], 0).astype(bf16)
    for s, o in enumerate((o0, o1, o2, o3)):
        o[...] = pay[low ^ s]


def pair_states(s0, s1, s2, s3, own, got, own_out, send_out, pair, states, starts):
    core, low, high, _ = places()
    pair[core] = own[...]
    pair[1 - core] = got[...]
    for s, ref in enumerate((s0, s1, s2, s3)):
        starts[low ^ s ^ (2 * high)] = ref[...]
    for j in range(own.shape[0]):
        c, d, b, _, last = parse_wide(pair[0, j])
        link = jnp.where(last == parse_wide(pair[1, j])[3], 1.0, 0.0)
        start = starts[j, :DK]
        states[0, j] = starts[j]
        states[1, j, :DK] = (link * (c * start.astype(f32) - mm_left(d, start) + b)).astype(bf16)
        states[1, j, DK:] = starts[j, DK:]
    own_out[...] = states[core]
    send_out[...] = states[1 - core]


def project(own, got, local, read, silu, w, acc, o1, o2, o3, tail, normed, total, lasts):
    core = places()[0]
    x = lax.axis_index("head")
    half = own.shape[0]
    width = half * DV
    for part, states in enumerate((own, got)):
        gated = []
        for h in range(half):
            at = part * half + h
            attention = local[at] + mm_left(read[at], states[h, :DK])
            mean_square = jnp.mean(attention * attention, axis=-1, keepdims=True)
            weight = lax.rsqrt(mean_square + EPS) * silu[:, at * DV : (at + 1) * DV]
            gated.append((attention * weight).astype(bf16))
            rows = states[h, DK:].astype(f32)
            lasts[(core ^ part) * half + h] = jnp.concatenate([rows[:4] + rows[4:8], rows[8:12]], 0)
        first = pl.multiple_of((core ^ part) * width, width)
        normed[:, pl.ds(first, width)] = jnp.concatenate(gated, 1)
    finals = []
    for h in range(2 * half):
        rows = lasts[h]
        finals.append(jnp.where(core == 0, rows[0:2], rows[2:4]))
    finals = jnp.concatenate(finals, 0)
    hi = finals.astype(bf16).astype(f32)
    tail[...] = jnp.concatenate([hi, finals - hi], 0).astype(bf16)
    total[...] = mm(normed[...], w[...])
    acc[...] = total[pl.ds(x * 32, 32)]
    width = total.shape[1]
    for s, o in enumerate((o1, o2, o3)):
        o[:, :width] = total[pl.ds((x ^ (s + 1)) * 32, 32)].astype(bf16)
        o[:, width:] = tail[...]


def finish(order, acc, r1, r2, r3, tail, out, decode, final):
    x = lax.axis_index("head")
    total = acc[...]
    width = total.shape[1]
    for r in (r1, r2, r3):
        total = total + r[:, :width].astype(f32)
    out[...] = total.astype(bf16)
    slots = decode.shape[0]
    for s, block in enumerate((tail[...], r1[:, width:], r2[:, width:], r3[:, width:])):
        block = block.astype(f32)
        rows = block[:16] + block[16:]
        for h in range(slots):
            line = jnp.concatenate([rows[2 * h : 2 * h + 1], rows[2 * h + 1 : 2 * h + 2]], 1)
            final[pl.ds((x ^ s) * slots + h, 1)] = line
    for i in range(slots):
        decode[i : i + 1] = final[pl.ds(order[x * slots + i], 1)]


def shape(dims, dtype=bf16):
    return pltpu.VMEM(dims, dtype)


def call(kernel, outs, scratch, *args, smem=0, hbm=(), flops=None):
    specs = [pl.BlockSpec(memory_space=pltpu.SMEM)] * smem
    specs += [
        pl.BlockSpec(memory_space=pltpu.HBM if i in hbm else pltpu.VMEM) for i in range(smem, len(args))
    ]
    args = [
        a if i < smem else pltpu.with_memory_space_constraint(a, pltpu.HBM if i in hbm else pltpu.VMEM)
        for i, a in enumerate(args)
    ]
    cost = None if flops is None else pl.CostEstimate(flops=flops, transcendentals=0, bytes_accessed=0)
    return pl.pallas_call(
        kernel,
        out_shape=outs,
        scratch_shapes=scratch,
        in_specs=specs,
        cost_estimate=cost,
        compiler_params=pltpu.CompilerParams(vmem_limit_bytes=24 * 2**20),
    )(*args)


def xor_peers(count, bit):
    return [(i, i ^ bit) for i in range(count)]


def per_device(
    queries, keys, values, out_gate, log_decay, write_strength, segment_ids, head_order, out_weight
):
    heads = values.shape[1] // DV
    half = heads // 2
    peers = lax.axis_size("ctx")
    model = out_weight.shape[1]
    wide = (N + 8, 256)
    block = (ROWS, 256)
    block3 = (ROWS, 256)
    seg = segment_ids.reshape(1, N)
    maps = [
        shape((half,) + wide, f32),
        shape((half, N, N), f32),
        shape((half, N, 256), f32),
        shape((N, N), f32),
    ]
    inputs = (keys, values, log_decay.T, write_strength.T, seg)
    send, mixes1, both1, sums1, *held = call(
        send_maps,
        maps + [shape(a.shape, a.dtype) for a in inputs],
        [pltpu.SemaphoreType.DMA((5,))],
        *inputs,
        hbm=range(5),
    )
    got = lax.ppermute(send, "ctx", xor_peers(peers, 1))
    own, mixes0, both0, sums0 = call(own_maps, maps, [], *held, flops=10**9)
    m0, m1, m2, m3 = call(
        pair_maps,
        [shape(block)] * 4,
        [pltpu.VMEM((2, half) + wide, f32)],
        own, got,
    )
    m1, m2, m3 = [lax.ppermute(m, "ctx", xor_peers(peers, 2 * s)) for s, m in ((1, m1), (2, m2), (3, m3))]
    local, read, silu = call(
        local_reads,
        [shape((heads, N, DV), f32), shape((heads, N, DK), f32), shape((N, heads * DV), f32)],
        [],
        mixes0, both0, sums0, mixes1, both1, sums1, queries, held[0], held[4], out_gate,
        flops=2 * 10**9,
    )
    total, prefix, prefix_row = call(
        quad_maps,
        [shape(block3), shape((3, DK, 256), f32), shape((3, 8, DK), f32)],
        [pltpu.VMEM((4,) + block, bf16)],
        m0, m1, m2, m3,
    )
    total_got = lax.ppermute(total, "ctx", xor_peers(peers, 12))
    r0 = call(
        row_map,
        shape(block3),
        [pltpu.VMEM((2,) + block3, bf16)],
        total, total_got,
    )
    rows = [[(i, (i + 16 * s) % peers) for i in range(peers)] for s in (1, 2, 3)]
    rows[2] = [(i, i - 16) for i in range(peers // 2, peers)]
    r1, r2, r3 = [lax.ppermute(r0, "ctx", pairs) for pairs in rows]
    s0, s1, s2, s3 = call(
        scan_states,
        [shape((ROWS, DV))] * 4,
        [
            pltpu.VMEM((4,) + block3, bf16),
            pltpu.VMEM((2,) + block3, bf16),
            pltpu.VMEM((DK, DV), f32),
            pltpu.VMEM((4, ROWS, DV), bf16),
        ],
        r0, r1, r2, r3, total, total_got, prefix, prefix_row,
    )
    s1, s2, s3 = [lax.ppermute(m, "ctx", xor_peers(peers, 2 * s)) for s, m in ((1, s1), (2, s2), (3, s3))]
    own_state, send_state = call(
        pair_states,
        [shape((half, ROWS, DV))] * 2,
        [
            pltpu.VMEM((2, half) + wide, f32),
            pltpu.VMEM((2, half, ROWS, DV), bf16),
            pltpu.VMEM((half, ROWS, DV), bf16),
        ],
        s0, s1, s2, s3, own, got,
    )
    got_state = lax.ppermute(send_state, "ctx", xor_peers(peers, 1))
    acc, o1, o2, o3, tail = call(
        project,
        [shape((32, model), f32)] + [shape((32, model + DV))] * 3 + [shape((32, DV))],
        [
            pltpu.VMEM((N, heads * DV), bf16),
            pltpu.VMEM((N, model), f32),
            pltpu.VMEM((heads, 8, DV), f32),
        ],
        own_state, got_state, local, read, silu, out_weight,
    )
    o1, o2, o3 = [lax.ppermute(o, "head", xor_peers(4, s)) for s, o in ((1, o1), (2, o2), (3, o3))]
    return call(
        finish,
        [jax.ShapeDtypeStruct((32, model), bf16), jax.ShapeDtypeStruct((heads, 256), f32)],
        [pltpu.VMEM((4 * heads, 256), f32)],
        head_order, acc, o1, o2, o3, tail,
        smem=1,
    )


def solution(mesh):
    in_specs = (
        P("ctx", "head"),
        P("ctx", "head"),
        P("ctx", "head"),
        P("ctx", "head"),
        P("ctx", "head"),
        P("ctx", "head"),
        P("ctx"),
        P(),
        P("head", None),
    )
    out_specs = (P(("ctx", "head"), None), P("head", "ctx"))

    def run(*args):
        return tuple(per_device(*args))

    return jax.shard_map(run, mesh=mesh, in_specs=in_specs, out_specs=out_specs, check_vma=False)
```

```python
import jax
import jax.numpy as jnp
from jax import lax
from jax.experimental import pallas as pl
from jax.experimental.pallas import tpu as pltpu
from jax.sharding import PartitionSpec as P


f32 = jnp.float32
bf16 = jnp.bfloat16
DK = 128
DV = 128
N = 128
ROWS = N + 16
EPS = 1e-06


def mm(a, b):
    return jnp.dot(a, b, preferred_element_type=f32)


def split(x):
    hi = x.astype(bf16)
    return hi, (x - hi.astype(f32)).astype(bf16)


def mm_left(a, b):
    hi, lo = split(a)
    return mm(jnp.concatenate([hi, lo], 1), jnp.concatenate([b, b], 0))


def mm_right(a, b):
    hi, lo = split(b)
    return mm(jnp.concatenate([a, a], 1), jnp.concatenate([hi, lo], 0))


def mm_both(a, b):
    ah, al = split(a)
    bh, bl = split(b)
    return mm(jnp.concatenate([ah, al], 1), jnp.concatenate([bh, bh], 0)) + mm(ah, bl)


def iota(shape, axis):
    return lax.broadcasted_iota(jnp.int32, shape, axis)


def places():
    ctx = lax.axis_index("ctx")
    return ctx % 2, (ctx // 2) % 4, (ctx // 8) % 2, ctx // 16


def lines(shape, values):
    row = iota(shape, 0)
    out = jnp.zeros(shape, f32)
    for i, value in enumerate(values):
        out = jnp.where(row == i, jnp.broadcast_to(value[:, :1], shape), out)
    return out


def pack_wide(ref, at, c, d, b, first, last):
    ref[at + (pl.ds(0, N), pl.ds(0, DK))] = d
    ref[at + (pl.ds(0, N), pl.ds(DK, DV))] = b
    ref[at + (pl.ds(N, 8), slice(None))] = lines((8, 256), (c, first, last))


def parse_wide(block):
    tail = block[N:, :DK]
    return tail[0:1], block[:N, :DK], block[:N, DK:], tail[1:2], tail[2:3]


def pack(ref, c, d, b, first, last):
    c0 = c.astype(bf16).astype(f32)
    c1 = (c - c0).astype(bf16).astype(f32)
    ref[:N, :DK] = d.astype(bf16)
    hi = b.astype(bf16)
    ref[:N, DK : 2 * DK] = hi
    if ref.shape[1] > 2 * DK:
        ref[:N, 2 * DK :] = (b - hi.astype(f32)).astype(bf16)
    ref[N:] = lines((16, ref.shape[1]), (c0, c1, c - c0 - c1, first, last)).astype(bf16)


def parse(block):
    tail = block[N:, :DK].astype(f32)
    c = tail[0:1] + tail[1:2] + tail[2:3]
    b = block[:N, DK : 2 * DK].astype(f32)
    if block.shape[1] > 2 * DK:
        b = b + block[:N, 2 * DK :].astype(f32)
    return c, block[:N, :DK], b, tail[3:4], tail[4:5]


def times(d, x):
    return mm_right(d, x) if d.dtype == bf16 else mm_both(d, x)


def compose(earlier, later):
    ce, de, be, fe, le = earlier
    cl, dl, bl, fl, ll = later
    link = jnp.where(le == fl, 1.0, 0.0)
    de = de.astype(f32)
    moved = times(dl, jnp.concatenate([de, be], 1))
    cl = cl * link
    d = cl * de + (link * ce) * dl.astype(f32) - link * moved[:, :DK]
    b = cl * be - link * moved[:, DK:] + bl
    return cl * ce, d, b, fe, ll


def apply_map(parts, link, state):
    c, d, b = parts[:3]
    return link * (c * state - times(d, state) + b)


def inverses(couplings):
    ii, jj = iota((N, N), 0), iota((N, N), 1)
    eye = jnp.where(ii == jj, 1.0, 0.0)
    inside = (ii // 16) == (jj // 16)
    squared = [jnp.where(inside, c, 0.0) for c in couplings]
    inv = [eye - s for s in squared]
    for _ in range(3):
        squared = [mm_both(s, s) for s in squared]
        inv = [x + mm_both(x, s) for x, s in zip(inv, squared)]
    for size in (16, 32, 64):
        odd = range(size, N, 2 * size)
        sibling = (ii // (2 * size)) == (jj // (2 * size))
        ring = sibling & ((ii // size) != (jj // size))

        def take(x):
            return jnp.concatenate([x[r : r + size] for r in odd], 0)

        def spread(x):
            gap = jnp.zeros((size, N), f32)
            return jnp.concatenate([y for i in range(len(odd)) for y in (gap, x[i * size : (i + 1) * size])], 0)

        below = [mm_both(take(jnp.where(ring, c, 0.0)), x) for c, x in zip(couplings, inv)]
        inv = [x - spread(mm_both(take(x), spread(y))) for x, y in zip(inv, below)]
    return inv


def unit(x):
    x = x.astype(f32)
    return lax.rsqrt(jnp.sum(x * x, axis=-1, keepdims=True) + EPS)


def local_maps(heads, k_ref, v_ref, g_ref, b_ref, seg_ref, out, mixes, both, sums, v_wait=None):
    groups = heads // 2
    ii, jj = iota((N, N), 0), iota((N, N), 1)
    doc_row = jnp.broadcast_to(seg_ref[...].astype(f32), (N, N))
    doc_col = doc_row.T
    same = (doc_row == doc_col) & (ii >= jj)
    strict = same & (ii > jj)
    cont_row = doc_row[0:1] == doc_col[0:1]
    last_col = doc_col[:, 0:1] == doc_row[:, N - 1 : N]
    first_doc, last_doc = doc_col[0:1], doc_col[N - 1 : N]
    upper = jnp.where(ii <= jj, 1.0, 0.0).astype(bf16)
    count = out.shape[0]
    g = g_ref[pl.ds(heads, count)]
    beta = b_ref[pl.ds(heads, count)]
    g = jnp.concatenate([g, jnp.zeros((8 - count, N), f32)], 0)
    g0 = g.astype(bf16)
    g1 = (g - g0.astype(f32)).astype(bf16)
    g2 = (g - g0.astype(f32) - g1.astype(f32)).astype(bf16)
    rows = mm(g0, upper) + mm(g1, upper) + mm(g2, upper)
    ks = [k_ref[:, pl.ds(pl.multiple_of((groups + i) * DK, DK), DK)] for i in range(count // 2)]
    cols = jnp.concatenate([rows, beta, jnp.zeros((N - 8 - count, N), f32)], 0).T
    cum = cols[:, :count]
    rk = [unit(k) for k in ks]
    rk_row = [jnp.broadcast_to(r, (N, N)).T[0:1] for r in rk]
    kts = [k.astype(f32).T.astype(bf16) for k in ks]
    kk = [mm(k, kt) for k, kt in zip(ks, kts)]
    couplings = []
    sums[...] = cols
    for h in range(count):
        i = h // 2
        gap = cum[:, h : h + 1] - rows[h : h + 1]
        mix = jnp.where(same, jnp.exp(jnp.minimum(gap, 0.0)), 0.0) * rk_row[i]
        couplings.append(jnp.where(strict, (cols[:, 8 + h : 9 + h] * rk[i]) * (mix * kk[i]), 0.0))
        mixes[h] = mix
    inv = inverses(couplings)
    if v_wait:
        v_wait()
    for h in range(count):
        i = h // 2
        entry_row = jnp.where(cont_row, jnp.exp(rows[h : h + 1]), 0.0)
        beta_row = beta[h : h + 1]
        weighted = mm_left(inv[h] * (beta_row * entry_row * rk_row[i]), ks[i])
        pseudo = mm_left(inv[h] * beta_row, v_ref[:, pl.ds(pl.multiple_of((heads + h) * DV, DV), DV)])
        pair = jnp.concatenate([weighted, pseudo], 1)
        both[h] = pair
        last_gap = jnp.minimum(cum[N - 1 : N, h : h + 1] - cum[:, h : h + 1], 0.0)
        last_keys = jnp.where(last_col, jnp.exp(last_gap), 0.0) * rk[i]
        written = mm_right(kts[i], last_keys * pair)
        pack_wide(out, (h,), entry_row[:, N - 1 :], written[:, :DK], written[:, DK:], first_doc, last_doc)


def send_maps(k, v, g, b, seg, out, mixes, both, sums, k_in, v_in, g_in, b_in, seg_in, sems):
    moves = [
        pltpu.make_async_copy(src, dst, sems.at[i])
        for i, (src, dst) in enumerate(((k, k_in), (seg, seg_in), (g, g_in), (b, b_in), (v, v_in)))
    ]
    for move in moves:
        move.start()
    for move in moves[:4]:
        move.wait()
    heads = (1 - places()[0]) * out.shape[0]
    local_maps(heads, k_in, v_in, g_in, b_in, seg_in, out, mixes, both, sums, moves[4].wait)


def own_maps(k, v, g, b, seg, out, mixes, both, sums):
    local_maps(places()[0] * out.shape[0], k, v, g, b, seg, out, mixes, both, sums)


def local_reads(mixes0, both0, sums0, mixes1, both1, sums1, q_ref, k_ref, seg_ref, gate, local, read, silu):
    core = places()[0]
    half = mixes0.shape[0]
    width = half * DV
    docs = jnp.broadcast_to(seg_ref[...].astype(f32), (N, N))
    cont_col = docs.T[:, 0:1] == docs[:, 0:1]
    for part, (mixes, both, sums) in enumerate(((mixes0, both0, sums0), (mixes1, both1, sums1))):
        first = (core ^ part) * half
        for h in range(half):
            if h % 2 == 0:
                lanes = pl.ds(pl.multiple_of((first // 2 + h // 2) * DK, DK), DK)
                q = q_ref[:, lanes]
                rq = unit(q) * DK ** (-0.5)
                qk = rq * lax.dot_general(q, k_ref[:, lanes], (((1,), (1,)), ((), ())), preferred_element_type=f32)
            at = part * half + h
            mixed = mm_both(mixes[h] * qk, both[h])
            entry_col = jnp.where(cont_col, jnp.exp(sums[:, h : h + 1]), 0.0)
            local[at] = mixed[:, DK:]
            read[at] = (entry_col * rq) * q.astype(f32) - mixed[:, :DK]
        first = pl.multiple_of(first * DV, width)
        z = gate[:, pl.ds(first, width)].astype(f32)
        silu[:, part * width : (part + 1) * width] = z / (1.0 + jnp.exp(-z))


def pair_maps(own, got, *refs):
    outs, pair = refs[:4], refs[4]
    core, low, high, _ = places()
    pair[core] = own[...]
    pair[1 - core] = got[...]
    for s in range(4):
        j = low ^ s ^ (2 * high)
        pack(outs[s], *compose(parse_wide(pair[0, j]), parse_wide(pair[1, j])))


def quad_maps(m0, m1, m2, m3, total, prefix, prefix_row, maps):
    low = places()[1]
    for s, m in enumerate((m0, m1, m2, m3)):
        maps[low ^ s] = m[...]
    parts = [parse(maps[t]) for t in range(4)]
    wide = [(c, d.astype(f32), b, first, last) for c, d, b, first, last in parts]
    two = compose(wide[0], parts[1])
    pack(total, *compose(two, compose(wide[2], parts[3])))
    row = iota((8, DK), 0)
    for t, reached in enumerate((wide[0], two, compose(two, parts[2]))):
        prefix[t, :, :DK] = reached[1]
        prefix[t, :, DK:] = reached[2]
        link = jnp.where(reached[4] == parts[t + 1][3], 1.0, 0.0)
        prefix_row[t] = jnp.where(row == 0, reached[0], link)


def row_map(own, got, out, maps):
    high = places()[2]
    maps[high] = own[...]
    maps[1 - high] = got[...]
    pack(out, *compose(parse(maps[0]), parse(maps[1])))


def scan_states(r0, r1, r2, r3, own, got, prefix, prefix_row, o0, o1, o2, o3, maps, halves, final, pay):
    _, low, high, y = places()
    for s, r in enumerate((r0, r1, r2, r3)):
        maps[(y + 4 - s) % 4] = r[...]
    halves[high] = own[...]
    halves[1 - high] = got[...]

    def after(newer, older, there):
        link = jnp.where(older[4] == newer[3], there, 0.0)
        return apply_map(newer, 1.0, link * older[2])

    row = parse(maps[y])
    last, older = parse(maps[(y + 3) % 4]), parse(maps[(y + 2) % 4])
    reached = after(last, older, jnp.where(y >= 2, 1.0, 0.0))
    incoming = jnp.where(last[4] == row[3], jnp.where(y >= 1, 1.0, 0.0), 0.0) * reached
    final[...] = after(parse(maps[3]), parse(maps[2]), 1.0)
    first_half = parse(halves[0])
    link = jnp.where(first_half[4] == parse(halves[1])[3], 1.0, 0.0)
    start = jnp.where(high == 1, apply_map(first_half, link, incoming), incoming)
    for t in range(4):
        here = start
        if t:
            c, link = prefix_row[t - 1, 0:1], prefix_row[t - 1, 1:2]
            here = apply_map((c, prefix[t - 1, :, :DK], prefix[t - 1, :, DK:]), link, start)
        pay[t, :DK] = here.astype(bf16)
        rows = final[pl.ds(4 * (y * 8 + high * 4 + t), 4)]
        hi = rows.astype(bf16).astype(f32)
        pay[t, DK:] = jnp.concatenate([hi, rows - hi, jnp.zeros((8, DV), f32)], 0).astype(bf16)
    for s, o in enumerate((o0, o1, o2, o3)):
        o[...] = pay[low ^ s]


def pair_states(s0, s1, s2, s3, own, got, own_out, send_out, pair, states, starts):
    core, low, high, _ = places()
    pair[core] = own[...]
    pair[1 - core] = got[...]
    for s, ref in enumerate((s0, s1, s2, s3)):
        starts[low ^ s ^ (2 * high)] = ref[...]
    for j in range(own.shape[0]):
        c, d, b, _, last = parse_wide(pair[0, j])
        link = jnp.where(last == parse_wide(pair[1, j])[3], 1.0, 0.0)
        start = starts[j, :DK]
        states[0, j] = starts[j]
        states[1, j, :DK] = (link * (c * start.astype(f32) - mm_left(d, start) + b)).astype(bf16)
        states[1, j, DK:] = starts[j, DK:]
    own_out[...] = states[core]
    send_out[...] = states[1 - core]


def gated_heads(part, states, local, read, silu):
    half = states.shape[0]
    gated = []
    for h in range(half):
        at = part * half + h
        attention = local[at] + mm_left(read[at], states[h, :DK])
        mean_square = jnp.mean(attention * attention, axis=-1, keepdims=True)
        weight = lax.rsqrt(mean_square + EPS) * silu[:, at * DV : (at + 1) * DV]
        gated.append((attention * weight).astype(bf16))
    return jnp.concatenate(gated, 1)


def weight_rows(part, half):
    width = half * DV
    return pl.ds(pl.multiple_of((places()[0] ^ part) * width, width), width)


def project_own(own, local, read, silu, w, total):
    total[...] = mm(gated_heads(0, own, local, read, silu), w[weight_rows(0, own.shape[0])])


def project(own, got, begun, local, read, silu, w, acc, o1, o2, o3, tail, total, lasts):
    core = places()[0]
    x = lax.axis_index("head")
    half = own.shape[0]
    for part, states in enumerate((own, got)):
        for h in range(half):
            rows = states[h, DK:].astype(f32)
            lasts[(core ^ part) * half + h] = jnp.concatenate([rows[:4] + rows[4:8], rows[8:12]], 0)
    finals = []
    for h in range(2 * half):
        rows = lasts[h]
        finals.append(jnp.where(core == 0, rows[0:2], rows[2:4]))
    finals = jnp.concatenate(finals, 0)
    hi = finals.astype(bf16).astype(f32)
    tail[...] = jnp.concatenate([hi, finals - hi], 0).astype(bf16)
    total[...] = begun[...] + mm(gated_heads(1, got, local, read, silu), w[weight_rows(1, half)])
    acc[...] = total[pl.ds(x * 32, 32)]
    width = total.shape[1]
    for s, o in enumerate((o1, o2, o3)):
        o[:, :width] = total[pl.ds((x ^ (s + 1)) * 32, 32)].astype(bf16)
        o[:, width:] = tail[...]


def finish(order, acc, r1, r2, r3, tail, out, decode, final):
    x = lax.axis_index("head")
    total = acc[...]
    width = total.shape[1]
    for r in (r1, r2, r3):
        total = total + r[:, :width].astype(f32)
    out[...] = total.astype(bf16)
    slots = decode.shape[0]
    for s, block in enumerate((tail[...], r1[:, width:], r2[:, width:], r3[:, width:])):
        block = block.astype(f32)
        rows = block[:16] + block[16:]
        for h in range(slots):
            line = jnp.concatenate([rows[2 * h : 2 * h + 1], rows[2 * h + 1 : 2 * h + 2]], 1)
            final[pl.ds((x ^ s) * slots + h, 1)] = line
    for i in range(slots):
        decode[i : i + 1] = final[pl.ds(order[x * slots + i], 1)]


def shape(dims, dtype=bf16):
    return pltpu.VMEM(dims, dtype)


def call(kernel, outs, scratch, *args, smem=0, hbm=(), flops=None):
    specs = [pl.BlockSpec(memory_space=pltpu.SMEM)] * smem
    specs += [
        pl.BlockSpec(memory_space=pltpu.HBM if i in hbm else pltpu.VMEM) for i in range(smem, len(args))
    ]
    args = [
        a if i < smem else pltpu.with_memory_space_constraint(a, pltpu.HBM if i in hbm else pltpu.VMEM)
        for i, a in enumerate(args)
    ]
    cost = None if flops is None else pl.CostEstimate(flops=flops, transcendentals=0, bytes_accessed=0)
    return pl.pallas_call(
        kernel,
        out_shape=outs,
        scratch_shapes=scratch,
        in_specs=specs,
        cost_estimate=cost,
        compiler_params=pltpu.CompilerParams(vmem_limit_bytes=24 * 2**20),
    )(*args)


def move(x, axis, pairs):
    return lax.ppermute(x, axis, pairs)


def xor_peers(count, bit):
    return [(i, i ^ bit) for i in range(count)]


def per_device(
    queries, keys, values, out_gate, log_decay, write_strength, segment_ids, head_order, out_weight
):
    heads = values.shape[1] // DV
    half = heads // 2
    peers = lax.axis_size("ctx")
    model = out_weight.shape[1]
    wide = (N + 8, 256)
    block = (ROWS, 256)
    block3 = (ROWS, 256)
    seg = segment_ids.reshape(1, N)
    maps = [
        shape((half,) + wide, f32),
        shape((half, N, N), f32),
        shape((half, N, 256), f32),
        shape((N, N), f32),
    ]
    inputs = (keys, values, log_decay.T, write_strength.T, seg)
    send, mixes1, both1, sums1, *held = call(
        send_maps,
        maps + [shape(a.shape, a.dtype) for a in inputs],
        [pltpu.SemaphoreType.DMA((5,))],
        *inputs,
        hbm=range(5),
    )
    got = lax.ppermute(send, "ctx", xor_peers(peers, 1))
    own, mixes0, both0, sums0 = call(own_maps, maps, [], *held, flops=10**9)
    m0, m1, m2, m3 = call(
        pair_maps,
        [shape(block)] * 4,
        [pltpu.VMEM((2, half) + wide, f32)],
        own, got,
    )
    m1, m2, m3 = [move(m, "ctx", xor_peers(peers, 2 * s)) for s, m in ((1, m1), (2, m2), (3, m3))]
    local, read, silu = call(
        local_reads,
        [shape((heads, N, DV), f32), shape((heads, N, DK), f32), shape((N, heads * DV), f32)],
        [],
        mixes0, both0, sums0, mixes1, both1, sums1, queries, held[0], held[4], out_gate,
        flops=2 * 10**9,
    )
    total, prefix, prefix_row = call(
        quad_maps,
        [shape(block3), shape((3, DK, 256), f32), shape((3, 8, DK), f32)],
        [pltpu.VMEM((4,) + block, bf16)],
        m0, m1, m2, m3,
    )
    total_got = move(total, "ctx", xor_peers(peers, 12))
    r0 = call(
        row_map,
        shape(block3),
        [pltpu.VMEM((2,) + block3, bf16)],
        total, total_got,
    )
    rows = [[(i, (i + 16 * s) % peers) for i in range(peers)] for s in (1, 2, 3)]
    rows[2] = [(i, i - 16) for i in range(peers // 2, peers)]
    r1, r2, r3 = [move(r0, "ctx", pairs) for pairs in rows]
    s0, s1, s2, s3 = call(
        scan_states,
        [shape((ROWS, DV))] * 4,
        [
            pltpu.VMEM((4,) + block3, bf16),
            pltpu.VMEM((2,) + block3, bf16),
            pltpu.VMEM((DK, DV), f32),
            pltpu.VMEM((4, ROWS, DV), bf16),
        ],
        r0, r1, r2, r3, total, total_got, prefix, prefix_row,
    )
    s1, s2, s3 = [move(m, "ctx", xor_peers(peers, 2 * s)) for s, m in ((1, s1), (2, s2), (3, s3))]
    own_state, send_state = call(
        pair_states,
        [shape((half, ROWS, DV))] * 2,
        [
            pltpu.VMEM((2, half) + wide, f32),
            pltpu.VMEM((2, half, ROWS, DV), bf16),
            pltpu.VMEM((half, ROWS, DV), bf16),
        ],
        s0, s1, s2, s3, own, got,
    )
    got_state = move(send_state, "ctx", xor_peers(peers, 1))
    begun = call(
        project_own,
        shape((N, model), f32),
        [],
        own_state, local, read, silu, out_weight,
        flops=10**9,
    )
    acc, o1, o2, o3, tail = call(
        project,
        [shape((32, model), f32)] + [shape((32, model + DV))] * 3 + [shape((32, DV))],
        [
            pltpu.VMEM((N, model), f32),
            pltpu.VMEM((heads, 8, DV), f32),
        ],
        own_state, got_state, begun, local, read, silu, out_weight,
    )
    o1, o2, o3 = [move(o, "head", xor_peers(4, s)) for s, o in ((1, o1), (2, o2), (3, o3))]
    return call(
        finish,
        [jax.ShapeDtypeStruct((32, model), bf16), jax.ShapeDtypeStruct((heads, 256), f32)],
        [pltpu.VMEM((4 * heads, 256), f32)],
        head_order, acc, o1, o2, o3, tail,
        smem=1,
    )


def solution(mesh):
    in_specs = (
        P("ctx", "head"),
        P("ctx", "head"),
        P("ctx", "head"),
        P("ctx", "head"),
        P("ctx", "head"),
        P("ctx", "head"),
        P("ctx"),
        P(),
        P("head", None),
    )
    out_specs = (P(("ctx", "head"), None), P("head", "ctx"))

    def run(*args):
        return tuple(per_device(*args))

    return jax.shard_map(run, mesh=mesh, in_specs=in_specs, out_specs=out_specs, check_vma=False)
```

```python
import jax
import jax.numpy as jnp
from jax import lax
from jax.experimental import pallas as pl
from jax.experimental.pallas import tpu as pltpu
from jax.sharding import PartitionSpec as P


f32 = jnp.float32
bf16 = jnp.bfloat16
DK = 128
DV = 128
N = 128
ROWS = N + 16
EPS = 1e-06


def mm(a, b):
    return jnp.dot(a, b, preferred_element_type=f32)


def split(x):
    hi = x.astype(bf16)
    return hi, (x - hi.astype(f32)).astype(bf16)


def mm_left(a, b):
    hi, lo = split(a)
    return mm(jnp.concatenate([hi, lo], 1), jnp.concatenate([b, b], 0))


def mm_right(a, b):
    hi, lo = split(b)
    return mm(jnp.concatenate([a, a], 1), jnp.concatenate([hi, lo], 0))


def mm_both(a, b):
    ah, al = split(a)
    bh, bl = split(b)
    return mm(jnp.concatenate([ah, al], 1), jnp.concatenate([bh, bh], 0)) + mm(ah, bl)


def iota(shape, axis):
    return lax.broadcasted_iota(jnp.int32, shape, axis)


def places():
    ctx = lax.axis_index("ctx")
    return ctx % 2, (ctx // 2) % 4, (ctx // 8) % 2, ctx // 16


def lines(shape, values):
    row = iota(shape, 0)
    out = jnp.zeros(shape, f32)
    for i, value in enumerate(values):
        out = jnp.where(row == i, jnp.broadcast_to(value[:, :1], shape), out)
    return out


def pack_wide(ref, at, c, d, b, first, last):
    ref[at + (pl.ds(0, N), pl.ds(0, DK))] = d
    ref[at + (pl.ds(0, N), pl.ds(DK, DV))] = b
    ref[at + (pl.ds(N, 8), slice(None))] = lines((8, 256), (c, first, last))


def parse_wide(block):
    tail = block[N:, :DK]
    return tail[0:1], block[:N, :DK], block[:N, DK:], tail[1:2], tail[2:3]


def pack(ref, c, d, b, first, last):
    c0 = c.astype(bf16).astype(f32)
    c1 = (c - c0).astype(bf16).astype(f32)
    ref[:N, :DK] = d.astype(bf16)
    hi = b.astype(bf16)
    ref[:N, DK : 2 * DK] = hi
    if ref.shape[1] > 2 * DK:
        ref[:N, 2 * DK :] = (b - hi.astype(f32)).astype(bf16)
    ref[N:] = lines((16, ref.shape[1]), (c0, c1, c - c0 - c1, first, last)).astype(bf16)


def parse(block):
    tail = block[N:, :DK].astype(f32)
    c = tail[0:1] + tail[1:2] + tail[2:3]
    b = block[:N, DK : 2 * DK].astype(f32)
    if block.shape[1] > 2 * DK:
        b = b + block[:N, 2 * DK :].astype(f32)
    return c, block[:N, :DK], b, tail[3:4], tail[4:5]


def times(d, x):
    return mm_right(d, x) if d.dtype == bf16 else mm_both(d, x)


def compose(earlier, later):
    ce, de, be, fe, le = earlier
    cl, dl, bl, fl, ll = later
    link = jnp.where(le == fl, 1.0, 0.0)
    de = de.astype(f32)
    moved = times(dl, jnp.concatenate([de, be], 1))
    cl = cl * link
    d = cl * de + (link * ce) * dl.astype(f32) - link * moved[:, :DK]
    b = cl * be - link * moved[:, DK:] + bl
    return cl * ce, d, b, fe, ll


def apply_map(parts, link, state):
    c, d, b = parts[:3]
    return link * (c * state - times(d, state) + b)


def inverses(couplings):
    ii, jj = iota((N, N), 0), iota((N, N), 1)
    eye = jnp.where(ii == jj, 1.0, 0.0)
    inside = (ii // 16) == (jj // 16)
    squared = [jnp.where(inside, c, 0.0) for c in couplings]
    inv = [eye - s for s in squared]
    for _ in range(3):
        squared = [mm_both(s, s) for s in squared]
        inv = [x + mm_both(x, s) for x, s in zip(inv, squared)]
    for size in (16, 32, 64):
        odd = range(size, N, 2 * size)
        sibling = (ii // (2 * size)) == (jj // (2 * size))
        ring = sibling & ((ii // size) != (jj // size))

        def take(x):
            return jnp.concatenate([x[r : r + size] for r in odd], 0)

        def spread(x):
            gap = jnp.zeros((size, N), f32)
            return jnp.concatenate([y for i in range(len(odd)) for y in (gap, x[i * size : (i + 1) * size])], 0)

        below = [mm_both(take(jnp.where(ring, c, 0.0)), x) for c, x in zip(couplings, inv)]
        inv = [x - spread(mm_both(take(x), spread(y))) for x, y in zip(inv, below)]
    return inv


def unit(x):
    x = x.astype(f32)
    return lax.rsqrt(jnp.sum(x * x, axis=-1, keepdims=True) + EPS)


def local_maps(heads, k_ref, v_ref, g_ref, b_ref, seg_ref, out, mixes, both, sums, v_wait=None):
    groups = heads // 2
    ii, jj = iota((N, N), 0), iota((N, N), 1)
    doc_row = jnp.broadcast_to(seg_ref[...].astype(f32), (N, N))
    doc_col = doc_row.T
    same = (doc_row == doc_col) & (ii >= jj)
    strict = same & (ii > jj)
    cont_row = doc_row[0:1] == doc_col[0:1]
    last_col = doc_col[:, 0:1] == doc_row[:, N - 1 : N]
    first_doc, last_doc = doc_col[0:1], doc_col[N - 1 : N]
    upper = jnp.where(ii <= jj, 1.0, 0.0).astype(bf16)
    count = out.shape[0]
    g = g_ref[pl.ds(heads, count)]
    beta = b_ref[pl.ds(heads, count)]
    g = jnp.concatenate([g, jnp.zeros((8 - count, N), f32)], 0)
    g0 = g.astype(bf16)
    g1 = (g - g0.astype(f32)).astype(bf16)
    g2 = (g - g0.astype(f32) - g1.astype(f32)).astype(bf16)
    rows = mm(g0, upper) + mm(g1, upper) + mm(g2, upper)
    ks = [k_ref[:, pl.ds(pl.multiple_of((groups + i) * DK, DK), DK)] for i in range(count // 2)]
    cols = jnp.concatenate([rows, beta, jnp.zeros((N - 8 - count, N), f32)], 0).T
    cum = cols[:, :count]
    rk = [unit(k) for k in ks]
    rk_row = [jnp.broadcast_to(r, (N, N)).T[0:1] for r in rk]
    kts = [k.astype(f32).T.astype(bf16) for k in ks]
    kk = [mm(k, kt) for k, kt in zip(ks, kts)]
    couplings = []
    sums[...] = cols
    for h in range(count):
        i = h // 2
        gap = cum[:, h : h + 1] - rows[h : h + 1]
        mix = jnp.where(same, jnp.exp(jnp.minimum(gap, 0.0)), 0.0) * rk_row[i]
        couplings.append(jnp.where(strict, (cols[:, 8 + h : 9 + h] * rk[i]) * (mix * kk[i]), 0.0))
        mixes[h] = mix
    inv = inverses(couplings)
    if v_wait:
        v_wait()
    for h in range(count):
        i = h // 2
        entry_row = jnp.where(cont_row, jnp.exp(rows[h : h + 1]), 0.0)
        beta_row = beta[h : h + 1]
        weighted = mm_left(inv[h] * (beta_row * entry_row * rk_row[i]), ks[i])
        pseudo = mm_left(inv[h] * beta_row, v_ref[:, pl.ds(pl.multiple_of((heads + h) * DV, DV), DV)])
        pair = jnp.concatenate([weighted, pseudo], 1)
        both[h] = pair
        last_gap = jnp.minimum(cum[N - 1 : N, h : h + 1] - cum[:, h : h + 1], 0.0)
        last_keys = jnp.where(last_col, jnp.exp(last_gap), 0.0) * rk[i]
        written = mm_right(kts[i], last_keys * pair)
        pack_wide(out, (h,), entry_row[:, N - 1 :], written[:, :DK], written[:, DK:], first_doc, last_doc)


def send_maps(k, v, g, b, seg, out, mixes, both, sums, k_in, v_in, g_in, b_in, seg_in, sems):
    moves = [
        pltpu.make_async_copy(src, dst, sems.at[i])
        for i, (src, dst) in enumerate(((k, k_in), (seg, seg_in), (g, g_in), (b, b_in), (v, v_in)))
    ]
    for move in moves:
        move.start()
    for move in moves[:4]:
        move.wait()
    heads = (1 - places()[0]) * out.shape[0]
    local_maps(heads, k_in, v_in, g_in, b_in, seg_in, out, mixes, both, sums, moves[4].wait)


def own_maps(k, v, g, b, seg, out, mixes, both, sums):
    local_maps(places()[0] * out.shape[0], k, v, g, b, seg, out, mixes, both, sums)


def local_reads(mixes0, both0, sums0, mixes1, both1, sums1, q_ref, k_ref, seg_ref, gate, local, read, silu):
    core = places()[0]
    half = mixes0.shape[0]
    width = half * DV
    docs = jnp.broadcast_to(seg_ref[...].astype(f32), (N, N))
    cont_col = docs.T[:, 0:1] == docs[:, 0:1]
    for part, (mixes, both, sums) in enumerate(((mixes0, both0, sums0), (mixes1, both1, sums1))):
        first = (core ^ part) * half
        for h in range(half):
            if h % 2 == 0:
                lanes = pl.ds(pl.multiple_of((first // 2 + h // 2) * DK, DK), DK)
                q = q_ref[:, lanes]
                rq = unit(q) * DK ** (-0.5)
                qk = rq * lax.dot_general(q, k_ref[:, lanes], (((1,), (1,)), ((), ())), preferred_element_type=f32)
            at = part * half + h
            mixed = mm_both(mixes[h] * qk, both[h])
            entry_col = jnp.where(cont_col, jnp.exp(sums[:, h : h + 1]), 0.0)
            local[at] = mixed[:, DK:]
            read[at] = (entry_col * rq) * q.astype(f32) - mixed[:, :DK]
        first = pl.multiple_of(first * DV, width)
        z = gate[:, pl.ds(first, width)].astype(f32)
        silu[:, part * width : (part + 1) * width] = z / (1.0 + jnp.exp(-z))


def pair_maps(own, got, *refs):
    outs, pair = refs[:4], refs[4]
    core, low, high, _ = places()
    pair[core] = own[...]
    pair[1 - core] = got[...]
    for s in range(4):
        j = low ^ s ^ (2 * high)
        pack(outs[s], *compose(parse_wide(pair[0, j]), parse_wide(pair[1, j])))


def quad_maps(m0, m1, m2, m3, total, prefix, prefix_row, maps):
    low = places()[1]
    for s, m in enumerate((m0, m1, m2, m3)):
        maps[low ^ s] = m[...]
    parts = [parse(maps[t]) for t in range(4)]
    wide = [(c, d.astype(f32), b, first, last) for c, d, b, first, last in parts]
    two = compose(wide[0], parts[1])
    pack(total, *compose(two, compose(wide[2], parts[3])))
    row = iota((8, DK), 0)
    for t, reached in enumerate((wide[0], two, compose(two, parts[2]))):
        prefix[t, :, :DK] = reached[1]
        prefix[t, :, DK:] = reached[2]
        link = jnp.where(reached[4] == parts[t + 1][3], 1.0, 0.0)
        prefix_row[t] = jnp.where(row == 0, reached[0], link)


def row_map(own, got, out, maps):
    high = places()[2]
    maps[high] = own[...]
    maps[1 - high] = got[...]
    pack(out, *compose(parse(maps[0]), parse(maps[1])))


def scan_states(r0, r1, r2, r3, own, got, prefix, prefix_row, o0, o1, o2, o3, maps, halves, final, pay):
    _, low, high, y = places()
    for s, r in enumerate((r0, r1, r2, r3)):
        maps[(y + 4 - s) % 4] = r[...]
    halves[high] = own[...]
    halves[1 - high] = got[...]

    def after(newer, older, there):
        link = jnp.where(older[4] == newer[3], there, 0.0)
        return apply_map(newer, 1.0, link * older[2])

    row = parse(maps[y])
    last, older = parse(maps[(y + 3) % 4]), parse(maps[(y + 2) % 4])
    reached = after(last, older, jnp.where(y >= 2, 1.0, 0.0))
    incoming = jnp.where(last[4] == row[3], jnp.where(y >= 1, 1.0, 0.0), 0.0) * reached
    final[...] = after(parse(maps[3]), parse(maps[2]), 1.0)
    first_half = parse(halves[0])
    link = jnp.where(first_half[4] == parse(halves[1])[3], 1.0, 0.0)
    start = jnp.where(high == 1, apply_map(first_half, link, incoming), incoming)
    for t in range(4):
        here = start
        if t:
            c, link = prefix_row[t - 1, 0:1], prefix_row[t - 1, 1:2]
            here = apply_map((c, prefix[t - 1, :, :DK].astype(bf16), prefix[t - 1, :, DK:]), link, start)
        pay[t, :DK] = here.astype(bf16)
        rows = final[pl.ds(4 * (y * 8 + high * 4 + t), 4)]
        hi = rows.astype(bf16).astype(f32)
        pay[t, DK:] = jnp.concatenate([hi, rows - hi, jnp.zeros((8, DV), f32)], 0).astype(bf16)
    for s, o in enumerate((o0, o1, o2, o3)):
        o[...] = pay[low ^ s]


def pair_states(s0, s1, s2, s3, own, got, own_out, send_out, pair, states, starts):
    core, low, high, _ = places()
    pair[core] = own[...]
    pair[1 - core] = got[...]
    for s, ref in enumerate((s0, s1, s2, s3)):
        starts[low ^ s ^ (2 * high)] = ref[...]
    for j in range(own.shape[0]):
        c, d, b, _, last = parse_wide(pair[0, j])
        link = jnp.where(last == parse_wide(pair[1, j])[3], 1.0, 0.0)
        start = starts[j, :DK]
        states[0, j] = starts[j]
        states[1, j, :DK] = (link * (c * start.astype(f32) - mm_left(d, start) + b)).astype(bf16)
        states[1, j, DK:] = starts[j, DK:]
    own_out[...] = states[core]
    send_out[...] = states[1 - core]


def gated_heads(part, states, local, read, silu):
    half = states.shape[0]
    gated = []
    for h in range(half):
        at = part * half + h
        attention = local[at] + mm_left(read[at], states[h, :DK])
        mean_square = jnp.mean(attention * attention, axis=-1, keepdims=True)
        weight = lax.rsqrt(mean_square + EPS) * silu[:, at * DV : (at + 1) * DV]
        gated.append((attention * weight).astype(bf16))
    return jnp.concatenate(gated, 1)


def weight_rows(part, half):
    width = half * DV
    return pl.ds(pl.multiple_of((places()[0] ^ part) * width, width), width)


def project_own(own, local, read, silu, w, total):
    total[...] = mm(gated_heads(0, own, local, read, silu), w[weight_rows(0, own.shape[0])])


def project(own, got, begun, local, read, silu, w, acc, o1, o2, o3, tail, total, lasts):
    core = places()[0]
    x = lax.axis_index("head")
    half = own.shape[0]
    for part, states in enumerate((own, got)):
        for h in range(half):
            rows = states[h, DK:].astype(f32)
            lasts[(core ^ part) * half + h] = jnp.concatenate([rows[:4] + rows[4:8], rows[8:12]], 0)
    finals = []
    for h in range(2 * half):
        rows = lasts[h]
        finals.append(jnp.where(core == 0, rows[0:2], rows[2:4]))
    finals = jnp.concatenate(finals, 0)
    hi = finals.astype(bf16).astype(f32)
    tail[...] = jnp.concatenate([hi, finals - hi], 0).astype(bf16)
    total[...] = begun[...] + mm(gated_heads(1, got, local, read, silu), w[weight_rows(1, half)])
    acc[...] = total[pl.ds(x * 32, 32)]
    width = total.shape[1]
    for s, o in enumerate((o1, o2, o3)):
        o[:, :width] = total[pl.ds((x ^ (s + 1)) * 32, 32)].astype(bf16)
        o[:, width:] = tail[...]


def finish(order, acc, r1, r2, r3, tail, out, decode, final):
    x = lax.axis_index("head")
    total = acc[...]
    width = total.shape[1]
    for r in (r1, r2, r3):
        total = total + r[:, :width].astype(f32)
    out[...] = total.astype(bf16)
    slots = decode.shape[0]
    for s, block in enumerate((tail[...], r1[:, width:], r2[:, width:], r3[:, width:])):
        block = block.astype(f32)
        rows = block[:16] + block[16:]
        for h in range(slots):
            line = jnp.concatenate([rows[2 * h : 2 * h + 1], rows[2 * h + 1 : 2 * h + 2]], 1)
            final[pl.ds((x ^ s) * slots + h, 1)] = line
    for i in range(slots):
        decode[i : i + 1] = final[pl.ds(order[x * slots + i], 1)]


def shape(dims, dtype=bf16):
    return pltpu.VMEM(dims, dtype)


def call(kernel, outs, scratch, *args, smem=0, hbm=(), flops=None):
    specs = [pl.BlockSpec(memory_space=pltpu.SMEM)] * smem
    specs += [
        pl.BlockSpec(memory_space=pltpu.HBM if i in hbm else pltpu.VMEM) for i in range(smem, len(args))
    ]
    args = [
        a if i < smem else pltpu.with_memory_space_constraint(a, pltpu.HBM if i in hbm else pltpu.VMEM)
        for i, a in enumerate(args)
    ]
    cost = None if flops is None else pl.CostEstimate(flops=flops, transcendentals=0, bytes_accessed=0)
    return pl.pallas_call(
        kernel,
        out_shape=outs,
        scratch_shapes=scratch,
        in_specs=specs,
        cost_estimate=cost,
        compiler_params=pltpu.CompilerParams(vmem_limit_bytes=24 * 2**20),
    )(*args)


def xor_peers(count, bit):
    return [(i, i ^ bit) for i in range(count)]


def per_device(
    queries, keys, values, out_gate, log_decay, write_strength, segment_ids, head_order, out_weight
):
    heads = values.shape[1] // DV
    half = heads // 2
    peers = lax.axis_size("ctx")
    model = out_weight.shape[1]
    wide = (N + 8, 256)
    block = (ROWS, 256)
    block3 = (ROWS, 256)
    seg = segment_ids.reshape(1, N)
    maps = [
        shape((half,) + wide, f32),
        shape((half, N, N), f32),
        shape((half, N, 256), f32),
        shape((N, N), f32),
    ]
    inputs = (keys, values, log_decay.T, write_strength.T, seg)
    send, mixes1, both1, sums1, *held = call(
        send_maps,
        maps + [shape(a.shape, a.dtype) for a in inputs],
        [pltpu.SemaphoreType.DMA((5,))],
        *inputs,
        hbm=range(5),
    )
    got = lax.ppermute(send, "ctx", xor_peers(peers, 1))
    own, mixes0, both0, sums0 = call(own_maps, maps, [], *held, flops=10**9)
    m0, m1, m2, m3 = call(
        pair_maps,
        [shape(block)] * 4,
        [pltpu.VMEM((2, half) + wide, f32)],
        own, got,
    )
    m1, m2, m3 = [lax.ppermute(m, "ctx", xor_peers(peers, 2 * s)) for s, m in ((1, m1), (2, m2), (3, m3))]
    local, read, silu = call(
        local_reads,
        [shape((heads, N, DV), f32), shape((heads, N, DK), f32), shape((N, heads * DV), f32)],
        [],
        mixes0, both0, sums0, mixes1, both1, sums1, queries, held[0], held[4], out_gate,
        flops=2 * 10**9,
    )
    total, prefix, prefix_row = call(
        quad_maps,
        [shape(block3), shape((3, DK, 256), f32), shape((3, 8, DK), f32)],
        [pltpu.VMEM((4,) + block, bf16)],
        m0, m1, m2, m3,
    )
    total_got = lax.ppermute(total, "ctx", xor_peers(peers, 12))
    r0 = call(
        row_map,
        shape(block3),
        [pltpu.VMEM((2,) + block3, bf16)],
        total, total_got,
    )
    rows = [[(i, (i + 16 * s) % peers) for i in range(peers)] for s in (1, 2, 3)]
    rows[2] = [(i, i - 16) for i in range(peers // 2, peers)]
    r1, r2, r3 = [lax.ppermute(r0, "ctx", pairs) for pairs in rows]
    s0, s1, s2, s3 = call(
        scan_states,
        [shape((ROWS, DV))] * 4,
        [
            pltpu.VMEM((4,) + block3, bf16),
            pltpu.VMEM((2,) + block3, bf16),
            pltpu.VMEM((DK, DV), f32),
            pltpu.VMEM((4, ROWS, DV), bf16),
        ],
        r0, r1, r2, r3, total, total_got, prefix, prefix_row,
    )
    s1, s2, s3 = [lax.ppermute(m, "ctx", xor_peers(peers, 2 * s)) for s, m in ((1, s1), (2, s2), (3, s3))]
    own_state, send_state = call(
        pair_states,
        [shape((half, ROWS, DV))] * 2,
        [
            pltpu.VMEM((2, half) + wide, f32),
            pltpu.VMEM((2, half, ROWS, DV), bf16),
            pltpu.VMEM((half, ROWS, DV), bf16),
        ],
        s0, s1, s2, s3, own, got,
    )
    got_state = lax.ppermute(send_state, "ctx", xor_peers(peers, 1))
    begun = call(
        project_own,
        shape((N, model), f32),
        [],
        own_state, local, read, silu, out_weight,
        flops=10**9,
    )
    acc, o1, o2, o3, tail = call(
        project,
        [shape((32, model), f32)] + [shape((32, model + DV))] * 3 + [shape((32, DV))],
        [
            pltpu.VMEM((N, model), f32),
            pltpu.VMEM((heads, 8, DV), f32),
        ],
        own_state, got_state, begun, local, read, silu, out_weight,
    )
    o1, o2, o3 = [lax.ppermute(o, "head", xor_peers(4, s)) for s, o in ((1, o1), (2, o2), (3, o3))]
    return call(
        finish,
        [jax.ShapeDtypeStruct((32, model), bf16), jax.ShapeDtypeStruct((heads, 256), f32)],
        [pltpu.VMEM((4 * heads, 256), f32)],
        head_order, acc, o1, o2, o3, tail,
        smem=1,
    )


def solution(mesh):
    in_specs = (
        P("ctx", "head"),
        P("ctx", "head"),
        P("ctx", "head"),
        P("ctx", "head"),
        P("ctx", "head"),
        P("ctx", "head"),
        P("ctx"),
        P(),
        P("head", None),
    )
    out_specs = (P(("ctx", "head"), None), P("head", "ctx"))

    def run(*args):
        return tuple(per_device(*args))

    return jax.shard_map(run, mesh=mesh, in_specs=in_specs, out_specs=out_specs, check_vma=False)
```
